32 devices in a mesh: gx: 4 (over x, core), gy: 2 (over y), gz: 4 (over z).
Axes of the slice: x: 2, y: 2, z: 4, core: 2. Of those that a mesh axis runs over, the one named last changes fastest.
Arguments:
- grid_inputs: bfloat16 [186, 256, 256], P(None, 'gx', 'gy'), may hold values from -6 to 6
- embed_w1: bfloat16 [512, 186], replicated, may hold values from -0.4375 to 0.4375
- embed_b1: float32 [512], replicated, may hold values from -3 to 3
- embed_w2: bfloat16 [512, 512], replicated, may hold values from -0.25 to 0.25
- embed_gain: float32 [512], replicated, may hold values from 0.1 to 1.9
- edge_w1: bfloat16 [512, 1536], replicated, may hold values from -0.15625 to 0.15625
- edge_b1: float32 [512], replicated, may hold values from -3 to 3
- edge_w2: bfloat16 [512, 512], replicated, may hold values from -0.25 to 0.25
- message_gain: float32 [512], replicated, may hold values from 0.1 to 1.9
- message_bias: float32 [512], replicated, may hold values from -3 to 3
- mesh_latent: bfloat16 [512, 4, 2, 256], P('gz', 'gx', 'gy'), may hold values from -6 to 6
- edge_latent: bfloat16 [512, 4, 2, 2048], P('gz', 'gx', 'gy'), may hold values from -6 to 6
- senders: int32 [4, 2, 2048], P('gx', 'gy'), may hold values from 0 to 65535, as said below
- receivers: int32 [4, 2, 2048], P('gx', 'gy'), may hold values from 0 to 2047, as said below
- edge_counts: int32 [4, 2], P('gx', 'gy'), may hold values from 1 to 2048, as said below
Outputs:
- mesh_out: bfloat16 [512, 4, 2, 256], P('gz', 'gx', 'gy')
- grid_latent: bfloat16 [512, 256, 256], P('gz', 'gx', 'gy')
The draws below stay inside these ranges and needn't reach their ends.
Inputs may be any that keep to these rules, and one draw needn't show every extreme that they name: `senders`: an edge of tile (b, c) has its sender's row within 8 rows of rows b * 64 to (b + 1) * 64 - 1, clipped to the grid, and its column within 8 columns, cyclically, of columns c * 128 to (c + 1) * 128 - 1; this holds in every slot. `receivers`: an edge of tile t is received by a node of that tile, t * 256 to (t + 1) * 256 - 1, in every slot. `edge_counts`: the live edges of a tile are its first slots; some tile holds 2048 live edges.
All inputs are finite; a program needn't handle non-finite values.
Results may differ from the reference program's by a relative error of at most 0.0049.
Values may be sent and summed in bfloat16 or wider, within the bound.
A program may use at most 128 MiB of HBM per device.

```python
import jax
import jax.numpy as jnp
from jax import lax

LATENT = 512
CHANNELS = 186
GLAT = 64
GLON = 128
MESH_DEV = 256
EDGE_DEV = 2048
HALO = 8
BANDS = 4
SECTORS = 2
NLAT = 256
NLON = 256


def tile_coords():
    band_ids = jnp.arange(BANDS, dtype=jnp.int32)[:, None, None]
    sector_ids = jnp.arange(SECTORS, dtype=jnp.int32)[None, :, None]
    return (band_ids, sector_ids)


def draw_senders(key, part):
    band_ids, sector_ids = tile_coords()
    lat_key, lon_key = jax.random.split(jax.random.fold_in(key, 11))
    shape = (BANDS, SECTORS, EDGE_DEV)
    rows = jax.random.randint(lat_key, shape, 0, GLAT + 2 * HALO, dtype=jnp.int32) + band_ids * GLAT - HALO
    rows = jnp.clip(rows, 0, NLAT - 1)
    columns = jax.random.randint(lon_key, shape, 0, GLON + 2 * HALO, dtype=jnp.int32) + sector_ids * GLON - HALO + NLON
    columns = columns % NLON
    return (rows * NLON + columns).astype(jnp.int32)


def draw_receivers(key, part):
    band_ids, sector_ids = tile_coords()
    first_key, second_key = jax.random.split(jax.random.fold_in(key, 23))
    shape = (BANDS, SECTORS, EDGE_DEV)
    first = jax.random.randint(first_key, shape, 0, MESH_DEV, dtype=jnp.int32)
    second = jax.random.randint(second_key, shape, 0, MESH_DEV, dtype=jnp.int32)
    return ((band_ids * SECTORS + sector_ids) * MESH_DEV + jnp.minimum(first, second)).astype(jnp.int32)


def draw_edge_counts(key, part):
    band_ids = jnp.arange(BANDS, dtype=jnp.int32)[:, None]
    sector_ids = jnp.arange(SECTORS, dtype=jnp.int32)[None, :]
    distance = jnp.abs(2 * band_ids + 1 - BANDS)
    base = EDGE_DEV // 8 + (EDGE_DEV - EDGE_DEV // 8) * (distance - 1) * (distance - 1) // ((BANDS - 2) * (BANDS - 2))
    jitter_key, pick_key = jax.random.split(jax.random.fold_in(key, 37))
    jitter = jax.random.randint(jitter_key, (BANDS, SECTORS), 0, EDGE_DEV // 64 + 1, dtype=jnp.int32)
    chosen = jax.random.randint(pick_key, (BANDS, 1), 0, SECTORS, dtype=jnp.int32)
    jitter = jnp.where((distance == BANDS - 1) & (sector_ids == chosen), 0, jitter)
    return (base - jitter).astype(jnp.int32)


def steps_of(rng, dims, shards, smallest, top_value):
    loudness = 1.0
    for dim, blocks in shards:
        steps = jax.random.uniform(jax.random.fold_in(jax.random.fold_in(rng, 6), dim), (blocks,), jnp.float32, smallest / len(shards), top_value / len(shards))
        loudness = loudness * jnp.repeat(jnp.exp(steps), dims[dim] // blocks).reshape((-1,) + (1,) * (len(dims) - 1 - dim))
    return loudness


def normal_values(stream_key, dims, width, reach, cuts=(), kind=jnp.bfloat16):
    values = width * jax.random.normal(stream_key, dims, jnp.float32)
    if cuts:
        values = values * steps_of(stream_key, dims, cuts, -0.22, 0.18)
    return jnp.clip(values, -reach, reach).astype(kind)


def setup_inputs(seed: int = 0) -> dict:
    keys = jax.random.split(jax.random.key(seed), 16)
    return {
        "grid_inputs": normal_values(keys[0], (CHANNELS, NLAT, NLON), 1.0, 6.0, ((1, 4), (2, 2))),
        "embed_w1": normal_values(keys[1], (LATENT, CHANNELS), CHANNELS ** -0.5, 0.4375),
        "embed_b1": normal_values(keys[2], (LATENT,), 0.5, 3.0, (), jnp.float32),
        "embed_w2": normal_values(keys[3], (LATENT, LATENT), LATENT ** -0.5, 0.25),
        "embed_gain": jnp.clip(1.0 + 0.18 * jax.random.normal(keys[4], (LATENT,), jnp.float32), 0.1, 1.9),
        "edge_w1": normal_values(keys[5], (LATENT, 3 * LATENT), (3 * LATENT) ** -0.5, 0.15625),
        "edge_b1": normal_values(keys[6], (LATENT,), 0.5, 3.0, (), jnp.float32),
        "edge_w2": normal_values(keys[7], (LATENT, LATENT), LATENT ** -0.5, 0.25),
        "message_gain": jnp.clip(1.0 + 0.18 * jax.random.normal(keys[8], (LATENT,), jnp.float32), 0.1, 1.9),
        "message_bias": normal_values(keys[9], (LATENT,), 0.5, 3.0, (), jnp.float32),
        "mesh_latent": normal_values(keys[10], (LATENT, BANDS, SECTORS, MESH_DEV), 1.0, 6.0, ((0, 4), (1, 4), (2, 2))),
        "edge_latent": normal_values(keys[11], (LATENT, BANDS, SECTORS, EDGE_DEV), 1.0, 6.0, ((0, 4), (1, 4), (2, 2))),
        "senders": draw_senders(jax.random.fold_in(keys[15], 71), 0),
        "receivers": draw_receivers(jax.random.fold_in(keys[15], 71), 0),
        "edge_counts": draw_edge_counts(jax.random.fold_in(keys[15], 71), 0),
    }


epsilon = 1e-05

def normalize(values):
    average = lax.optimization_barrier(jnp.mean(values, axis=0, keepdims=True))
    centred = values - average
    spread = lax.optimization_barrier(jnp.mean(centred * centred, axis=0, keepdims=True))
    return centred * lax.rsqrt(spread + epsilon)

def reference(grid_inputs, embed_w1, embed_b1, embed_w2, embed_gain, edge_w1, edge_b1, edge_w2, message_gain, message_bias, mesh_latent, edge_latent, senders, receivers, edge_counts):
    band_inputs = grid_inputs.reshape(CHANNELS, BANDS, GLAT * NLON).transpose(1, 0, 2)

    def embed_band(block_inputs):
        hidden = jax.nn.silu(jnp.dot(embed_w1, block_inputs, preferred_element_type=jnp.float32) + embed_b1[:, None]).astype(jnp.bfloat16)
        first_pre = jnp.dot(embed_w2, hidden, preferred_element_type=jnp.float32)
        return (normalize(first_pre) * embed_gain[:, None]).astype(jnp.bfloat16)
    band_latent = lax.map(embed_band, band_inputs)
    grid_latent = band_latent.transpose(1, 0, 2).reshape(LATENT, NLAT * NLON)
    tile_count = BANDS * SECTORS
    node_total = tile_count * MESH_DEV
    mesh_flat = mesh_latent.reshape(LATENT, node_total)
    edge_tiles = edge_latent.reshape(LATENT, tile_count, EDGE_DEV).transpose(1, 0, 2)
    send_tiles = senders.reshape(tile_count, EDGE_DEV)
    recv_tiles = receivers.reshape(tile_count, EDGE_DEV)
    count_tiles = edge_counts.reshape(tile_count)
    slot_ids = jnp.arange(EDGE_DEV, dtype=jnp.int32)

    def tile_step(running, inputs):
        totals, degree = running
        edge_cols, send_ids, recv_ids, live_count = inputs
        live_mask = slot_ids < live_count
        stacked = jnp.concatenate([edge_cols, jnp.take(grid_latent, send_ids, axis=1), jnp.take(mesh_flat, recv_ids, axis=1)], axis=0)
        hidden = jax.nn.silu(jnp.dot(edge_w1, stacked, preferred_element_type=jnp.float32) + edge_b1[:, None]).astype(jnp.bfloat16)
        second = jnp.dot(edge_w2, hidden, preferred_element_type=jnp.float32)
        message = (edge_cols.astype(jnp.float32) + normalize(second) * message_gain[:, None] + message_bias[:, None]).astype(jnp.bfloat16)
        weights = jnp.where(live_mask[None, :], message.astype(jnp.float32), jnp.float32(0.0))
        totals = totals + jax.ops.segment_sum(weights.T, recv_ids, num_segments=node_total)
        degree = degree + jax.ops.segment_sum(live_mask.astype(jnp.int32), recv_ids, num_segments=node_total)
        return ((totals, degree), None)
    start_state = (jnp.zeros((node_total, LATENT), jnp.float32), jnp.zeros((node_total,), jnp.int32))
    (totals, degree), unused = lax.scan(tile_step, start_state, (edge_tiles, send_tiles, recv_tiles, count_tiles))
    scale = jnp.maximum(degree, 1).astype(jnp.float32)
    result = mesh_flat.astype(jnp.float32) + totals.T / scale[None, :]
    mesh_out = result.astype(jnp.bfloat16).reshape(LATENT, BANDS, SECTORS, MESH_DEV)
    return (mesh_out, grid_latent.reshape(LATENT, NLAT, NLON))
```

```python
import jax
import jax.numpy as jnp
from jax import lax
from jax.experimental import pallas as pl
from jax.experimental.pallas import tpu as pltpu
from jax.sharding import PartitionSpec as P

HALO = 8
ROWS = 16
GROUP = 4

epsilon = 1e-05
F32 = jnp.float32
BF16 = jnp.bfloat16


def half_silu(half):
    return half + half * jnp.tanh(half)


def centre(values):
    average = jnp.mean(values, axis=0, keepdims=True)
    centred = values - average
    spread = jnp.mean(centred * centred, axis=0, keepdims=True)
    return average, lax.rsqrt(spread + epsilon)


def onehot_of(index_row, first, count):
    ids = lax.broadcasted_iota(jnp.int32, (count, index_row.shape[1]), 0)
    return jnp.where(ids == index_row - first, 1.0, 0.0).astype(BF16)


MESH = pl.DeviceIdType.MESH


def partner(dx, dy, dz):
    ids = {}
    for axis, step in (("gx", dx), ("gy", dy), ("gz", dz)):
        size = lax.axis_size(axis)
        ids[axis] = lax.rem(lax.axis_index(axis) + (step + size), size)
    return ids


def split(values, size):
    if size & (size - 1) == 0:
        return lax.shift_right_logical(values, size.bit_length() - 1), values & (size - 1)
    return values // size, values % size


def locate(send, receive, live, near_ref, send_ref, nodes, lat, lon):
    band = lax.axis_index("gx")
    sector = lax.axis_index("gy")
    lon_total = lon * lax.axis_size("gy")
    slot_ids = lax.broadcasted_iota(jnp.int32, receive.shape, 1)
    tile = band * lax.axis_size("gy") + sector
    near_ref[...] = jnp.where(slot_ids < live, receive - tile * nodes, -1)
    row, column = split(send, lon_total)
    row = row - band * lat
    column = split(column - sector * lon + (HALO + lon_total), lon_total)[1] - HALO
    above, below = row < 0, row >= lat
    west, east = column < 0, column >= lon
    outside_row = jnp.where(above, 1, jnp.where(below, 1, 0))
    outside_column = jnp.where(west, 1, jnp.where(east, 1, 0))
    send_ref[0:1, :] = jnp.where(outside_row + outside_column == 0, row * lon + column, -1)
    strip = HALO * lon
    tall = lat * HALO
    row_index = jnp.where(above, row + HALO, row - lat + HALO) * lon + column
    beside = jnp.where(west, column + HALO, column - lon)
    column_index = 2 * strip + jnp.where(west, 0, tall) + row * HALO + beside
    corner = jnp.where(above, 0, 2) + jnp.where(west, 0, 1)
    corner_row = jnp.where(above, row + ROWS, row - lat)
    corner_index = 2 * (strip + tall) + (corner * ROWS + corner_row) * HALO + beside
    send_ref[1:2, :] = jnp.where(
        outside_column == 0,
        jnp.where(outside_row == 0, -1, row_index),
        jnp.where(outside_row == 0, column_index, corner_index),
    )


def kernel(
    x_hbm, w1_ref, w2_ref, e1_hbm, e2_hbm, b1_ref, gain_ref, eb1_ref, mgain_ref, mbias_ref,
    mesh_ref, edge_ref, senders_ref, receivers_ref, count_ref,
    stage, mean_ref,
    x_ref, wide, w1, cols, e1_ref, e2_ref, w1_wide, vec_ref, near_ref, send_ref, gathered, pre_ref, out_wide,
    rows_send, cols_send, rows_recv, cols_recv, corner_recv,
    assigned, nodes_all, totals, sent, parts,
    x_sem, w_sem, halo_send, halo_recv, z_send, z_recv,
):
    tiles, channels, rows, lon = x_ref.shape
    padded = w1.shape[1]
    latent, share = assigned.shape
    shard, nodes = mesh_ref.shape
    slots = edge_ref.shape[1]
    layers = slots // share
    me = lax.axis_index("gz")
    mine = pl.ds(pl.multiple_of(me * shard, shard), shard)

    diagonals = ((1, 1), (1, -1), (-1, 1), (-1, -1))
    around = [(1, 0, 0), (-1, 0, 0), (0, 1, 0), (0, -1, 0)]
    around += [(dx, dy, 0) for dx, dy in diagonals]
    around += [(0, 0, k) for k in range(1, layers)]
    barrier = pltpu.get_barrier_semaphore()
    for offset in around:
        pl.semaphore_signal(barrier, inc=1, device_id=partner(*offset), device_id_type=MESH)
    loads = [
        pltpu.make_async_copy(x_hbm.at[:, pl.ds(t * rows, rows), :], x_ref.at[t], x_sem.at[t])
        for t in range(tiles)
    ]
    weights = [
        pltpu.make_async_copy(e1_hbm, e1_ref, w_sem.at[0]),
        pltpu.make_async_copy(e2_hbm, e2_ref, w_sem.at[1]),
    ]
    for load in loads + weights:
        load.start()

    w1_wide[...] = jnp.zeros_like(w1_wide)
    w1_wide[:channels, :] = w1_ref[...].astype(F32) * 0.5
    w1[...] = w1_wide[...].T[:, :padded].astype(BF16)
    vec_ref[...] = jnp.zeros_like(vec_ref)
    for i, ref in enumerate((b1_ref, gain_ref, eb1_ref, mgain_ref, mbias_ref)):
        vec_ref[i : i + 1, :] = ref[...]
    cols[...] = vec_ref[...].T
    locate(
        senders_ref[:, pl.ds(pl.multiple_of(me * share, share), share)],
        receivers_ref[...], count_ref[0, 0], near_ref, send_ref, nodes, tiles * rows, lon,
    )
    send_ref[2:3, :] = near_ref[:, pl.ds(pl.multiple_of(me * share, share), share)]
    b1, gain = cols[:, 0:1] * 0.5, cols[:, 1:2]
    gathered[...] = jnp.zeros_like(gathered)
    assigned[mine, :] = edge_ref[:, pl.ds(pl.multiple_of(me * share, share), share)]
    nodes_all[mine, :] = mesh_ref[...]
    pl.semaphore_wait(barrier, len(around))

    def remote(source, target, send_sem, recv_sem, offset):
        return pltpu.make_async_remote_copy(
            src_ref=source, dst_ref=target, send_sem=send_sem, recv_sem=recv_sem,
            device_id=partner(*offset), device_id_type=MESH,
        )

    spread = []
    for k in range(1, layers):
        peer = lax.rem(me + k, layers)
        theirs = pl.ds(pl.multiple_of(peer * share, share), share)
        spread.append(
            remote(edge_ref.at[:, theirs], assigned.at[mine, :], z_send.at[0, k], z_recv.at[0, k], (0, 0, k))
        )
        spread.append(
            remote(mesh_ref, nodes_all.at[mine, :], z_send.at[1, k], z_recv.at[1, k], (0, 0, k))
        )
    for copy in spread:
        copy.start()

    def widen(t, carry):
        pltpu.make_async_copy(
            x_hbm.at[:, pl.ds(t * rows, rows), :], x_ref.at[t], x_sem.at[t]
        ).wait()
        wide[t, pl.ds(0, channels * rows), :] = x_ref[t].astype(F32).reshape(channels * rows, lon)
        wide[t, pl.ds(channels * rows, (padded - channels) * rows), :] = jnp.zeros(
            ((padded - channels) * rows, lon), F32
        )
        lanes = lax.broadcasted_iota(jnp.int32, (padded, lon), 1) // HALO
        left = jnp.zeros((padded, lon), F32)
        right = jnp.zeros((padded, lon), F32)
        for j in range(rows):
            row = wide[t, pl.ds(j, padded, stride=rows), :]
            here = lanes == j
            left = jnp.where(here, row if j == 0 else pltpu.roll(row, j * HALO, 1), left)
            turn = (j * HALO + HALO) % lon
            right = jnp.where(here, row if turn == 0 else pltpu.roll(row, turn, 1), right)
        cols_send[0, t] = left.astype(BF16)
        cols_send[1, t] = right.astype(BF16)
        return carry

    lax.fori_loop(0, tiles, widen, 0)
    for j in range(HALO):
        at = pl.ds(j * lon, lon)
        rows_send[0, :, at] = wide[0, pl.ds(j, padded, stride=rows), :].astype(BF16)
        rows_send[1, :, at] = wide[
            tiles - 1, pl.ds(rows - HALO + j, padded, stride=rows), :
        ].astype(BF16)

    def first_layer(t, group):
        cells = jnp.concatenate(
            [wide[t, pl.ds(group * GROUP + r, padded, stride=rows), :] for r in range(GROUP)],
            axis=1,
        ).astype(BF16)
        half = jnp.dot(w1[...], cells, preferred_element_type=F32) + b1
        return cells, half_silu(half).astype(BF16)

    def embed(t):
        own_gain = cols[mine, 1:2]
        cells, hidden = first_layer(t, 0)
        for group in range(rows // GROUP):
            slot = group % 2
            pre_ref[slot] = jnp.dot(w2_ref[...], hidden, preferred_element_type=F32)
            pick = onehot_of(send_ref[0:1, :], (t * rows + group * GROUP) * lon, GROUP * lon)
            gathered[...] += jnp.dot(cells, pick, preferred_element_type=F32)
            if (group + 1) * GROUP < rows:
                cells, hidden = first_layer(t, group + 1)
            average, scale = centre(pre_ref[slot])
            own = (pre_ref[slot, mine, :] - average) * scale * own_gain
            for r in range(GROUP):
                out_wide[pl.ds(group * GROUP + r, shard, stride=rows), :] = own[
                    :, r * lon : (r + 1) * lon
                ]
        stage[t] = out_wide[...].reshape(shard, rows, lon).astype(BF16)

    halo = [
        remote(rows_send.at[1], rows_recv.at[0], halo_send.at[0], halo_recv.at[0], (1, 0, 0)),
        remote(rows_send.at[0], rows_recv.at[1], halo_send.at[1], halo_recv.at[1], (-1, 0, 0)),
        remote(cols_send.at[1], cols_recv.at[0], halo_send.at[2], halo_recv.at[2], (0, 1, 0)),
        remote(cols_send.at[0], cols_recv.at[1], halo_send.at[3], halo_recv.at[3], (0, -1, 0)),
    ]
    for i, (dx, dy) in enumerate(diagonals):
        halo.append(
            remote(
                cols_send.at[1 if dy > 0 else 0, tiles - 1 if dx > 0 else 0],
                corner_recv.at[i], halo_send.at[4 + i], halo_recv.at[4 + i], (dx, dy, 0),
            )
        )
    for copy in halo:
        copy.start()

    def advance(t, carry):
        embed(t)
        return carry

    lax.fori_loop(0, tiles, advance, 0)

    for copy in halo:
        copy.wait()
    picked = gathered[...]
    first = 0
    pieces = [rows_recv[0], rows_recv[1]]
    pieces += [cols_recv[side, t] for side in range(2) for t in range(tiles)]
    pieces += [corner_recv[i] for i in range(4)]
    for piece in pieces:
        pick = onehot_of(send_ref[1:2, :], first, piece.shape[1])
        picked = picked + jnp.dot(piece, pick, preferred_element_type=F32)
        first += piece.shape[1]
    half = jnp.dot(w1[...], picked.astype(BF16), preferred_element_type=F32) + b1
    pre = jnp.dot(w2_ref[...], half_silu(half).astype(BF16), preferred_element_type=F32)
    average, scale = centre(pre)
    sender = ((pre - average) * scale * gain).astype(BF16)
    for copy in spread:
        copy.wait()
    onehot = onehot_of(send_ref[2:3, :], 0, nodes)
    mesh_cols = jnp.dot(nodes_all[...], onehot, preferred_element_type=F32).astype(BF16)
    for copy in weights:
        copy.wait()
    half = jnp.dot(e1_ref[:, :latent], assigned[...], preferred_element_type=F32)
    half = half + jnp.dot(e1_ref[:, latent : 2 * latent], sender, preferred_element_type=F32)
    half = half + jnp.dot(e1_ref[:, 2 * latent :], mesh_cols, preferred_element_type=F32)
    hidden = half_silu((half + cols[:, 2:3]) * 0.5).astype(BF16)
    second = jnp.dot(e2_ref[...], hidden, preferred_element_type=F32)
    average, scale = centre(second)
    message = (
        assigned[...].astype(F32) + (second - average) * scale * cols[:, 3:4] + cols[:, 4:5]
    ).astype(BF16)
    last = (((1,), (1,)), ((), ()))
    totals[...] = lax.dot_general(message, onehot, last, preferred_element_type=F32)
    sent[...] = totals[...].astype(BF16)
    exchange = []
    for k in range(1, layers):
        peer = lax.rem(me + k, layers)
        theirs = pl.ds(pl.multiple_of(peer * shard, shard), shard)
        exchange.append(
            remote(sent.at[theirs, :], parts.at[k], z_send.at[2, k], z_recv.at[2, k], (0, 0, k))
        )
    for copy in exchange:
        copy.start()
    degree = jnp.zeros((8, nodes), F32)
    for start in range(0, slots, share):
        chunk = onehot_of(near_ref[:, start : start + share], 0, nodes)
        ones = jnp.ones((8, share), BF16)
        degree = degree + lax.dot_general(ones, chunk, last, preferred_element_type=F32)
    scale = jnp.maximum(degree[:1], 1.0)
    for copy in exchange:
        copy.wait()
    total = totals[mine, :]
    for k in range(1, layers):
        total = total + parts[k].astype(F32)
    mean_ref[...] = (mesh_ref[...].astype(F32) + total / scale).astype(BF16)


def finish(stage, mesh_ref, grid_out, mesh_out, sem):
    tiles, _, rows, _ = stage.shape
    copies = [
        pltpu.make_async_copy(stage.at[t], grid_out.at[:, pl.ds(t * rows, rows), :], sem.at[t])
        for t in range(tiles)
    ]
    copies.append(pltpu.make_async_copy(mesh_ref, mesh_out, sem.at[tiles]))
    for copy in copies:
        copy.start()
    for copy in copies:
        copy.wait()


def on_device(
    grid_inputs,
    embed_w1,
    embed_b1,
    embed_w2,
    embed_gain,
    edge_w1,
    edge_b1,
    edge_w2,
    message_gain,
    message_bias,
    mesh_latent,
    edge_latent,
    senders,
    receivers,
    edge_counts,
):
    latent = embed_w2.shape[0]
    channels, lat, lon = grid_inputs.shape
    shard = mesh_latent.shape[0]
    nodes = mesh_latent.shape[3]
    slots = edge_latent.shape[3]
    layers = lax.axis_size("gz")
    share = slots // layers
    strip = HALO * lon
    padded = -(-channels // 16) * 16
    tiles = lat // ROWS

    vmem = pl.BlockSpec(memory_space=pltpu.VMEM)
    hbm = pl.BlockSpec(memory_space=pl.ANY)
    scratch = [
        ((tiles, channels, ROWS, lon), BF16),
        ((tiles, padded * ROWS, lon), F32),
        ((latent, padded), BF16),
        ((latent, 8), F32),
        (edge_w1.shape, BF16),
        (edge_w2.shape, BF16),
        ((-(-padded // 128) * 128, latent), F32),
        ((8, latent), F32),
        ((1, slots), jnp.int32),
        ((8, share), jnp.int32),
        ((padded, share), F32),
        ((2, latent, GROUP * lon), F32),
        ((shard * ROWS, lon), F32),
        ((2, padded, strip), BF16),
        ((2, tiles, padded, lon), BF16),
        ((2, padded, strip), BF16),
        ((2, tiles, padded, lon), BF16),
        ((4, padded, lon), BF16),
        ((latent, share), BF16),
        ((latent, nodes), BF16),
        ((latent, nodes), F32),
        ((latent, nodes), BF16),
        ((layers, shard, nodes), BF16),
    ]
    sems = [(tiles,), (2,), (8,), (8,), (3, layers), (3, layers)]
    smem = pl.BlockSpec(memory_space=pltpu.SMEM)
    line = lambda v: v.reshape(1, v.size)
    mesh_own = mesh_latent[:, 0, 0, :]
    stage, mean = pl.pallas_call(
        kernel,
        in_specs=[hbm, vmem, vmem, hbm, hbm] + [vmem] * 9 + [smem],
        out_specs=[vmem, vmem],
        out_shape=[
            pltpu.VMEM((tiles, shard, ROWS, lon), BF16),
            pltpu.VMEM((shard, nodes), BF16),
        ],
        scratch_shapes=[pltpu.VMEM(s, d) for s, d in scratch]
        + [pltpu.SemaphoreType.DMA(s) for s in sems],
        compiler_params=pltpu.CompilerParams(
            collective_id=0, has_side_effects=True, vmem_limit_bytes=60 * 1024 * 1024
        ),
    )(
        grid_inputs, embed_w1.T, embed_w2, edge_w1, edge_w2,
        line(embed_b1), line(embed_gain), line(edge_b1), line(message_gain), line(message_bias),
        mesh_own, edge_latent[:, 0, 0, :], line(senders), line(receivers), edge_counts,
    )
    grid_out, mesh_out = pl.pallas_call(
        finish,
        in_specs=[vmem, vmem],
        out_specs=[hbm, hbm],
        out_shape=[
            jax.ShapeDtypeStruct((shard, lat, lon), BF16),
            jax.ShapeDtypeStruct((shard, nodes), BF16),
        ],
        scratch_shapes=[pltpu.SemaphoreType.DMA((tiles + 1,))],
        compiler_params=pltpu.CompilerParams(vmem_limit_bytes=1024 * 1024),
    )(pltpu.with_memory_space_constraint(stage, pltpu.VMEM), pltpu.with_memory_space_constraint(mean, pltpu.VMEM))
    return (mesh_out.reshape(shard, 1, 1, nodes), grid_out)


def solution(mesh):
    return jax.shard_map(
        on_device,
        mesh=mesh,
        in_specs=(
            P(None, "gx", "gy"),
            P(),
            P(),
            P(),
            P(),
            P(),
            P(),
            P(),
            P(),
            P(),
            P("gz", "gx", "gy", None),
            P("gz", "gx", "gy", None),
            P("gx", "gy", None),
            P("gx", "gy", None),
            P("gx", "gy"),
        ),
        out_specs=(P("gz", "gx", "gy", None), P("gz", "gx", "gy")),
        check_vma=False,
    )
```

```python
import jax
import jax.numpy as jnp
from jax import lax
from jax.experimental import pallas as pl
from jax.experimental.pallas import tpu as pltpu
from jax.sharding import PartitionSpec as P

HALO = 8
ROWS = 16
GROUP = 4
EARLY = 2

epsilon = 1e-05
F32 = jnp.float32
BF16 = jnp.bfloat16
MESH = pl.DeviceIdType.MESH


def half_silu(half):
    return half + half * jnp.tanh(half)


def inverse_spread(values):
    return lax.rsqrt(jnp.mean(values * values, axis=0, keepdims=True) + epsilon)


def onehot_of(index_row, first, count):
    ids = lax.broadcasted_iota(jnp.int32, (count, index_row.shape[1]), 0)
    return jnp.where(ids == index_row - first, 1.0, 0.0).astype(BF16)


def partner(dx, dy, dz):
    ids = {}
    for axis, step in (("gx", dx), ("gy", dy), ("gz", dz)):
        size = lax.axis_size(axis)
        ids[axis] = lax.rem(lax.axis_index(axis) + (step + size), size)
    return ids


def remote(source, target, send_sem, recv_sem, offset):
    return pltpu.make_async_remote_copy(
        src_ref=source, dst_ref=target, send_sem=send_sem, recv_sem=recv_sem,
        device_id=partner(*offset), device_id_type=MESH,
    )


def split(values, size):
    if size & (size - 1) == 0:
        return lax.shift_right_logical(values, size.bit_length() - 1), values & (size - 1)
    return values // size, values % size


def locate(send, lat, lon, sides):
    band = lax.axis_index("gx")
    sector = lax.axis_index("gy")
    lon_total = lon * lax.axis_size("gy")
    row, column = split(send, lon_total)
    row = row - band * lat
    column = split(column - sector * lon + (HALO + lon_total), lon_total)[1] - HALO
    above, below = row < 0, row >= lat
    west, east = column < 0, column >= lon
    outside_row = jnp.where(above, 1, jnp.where(below, 1, 0))
    outside_column = jnp.where(west, 1, jnp.where(east, 1, 0))
    inside = outside_row + outside_column == 0
    strip = HALO * lon
    row_index = jnp.where(above, row + HALO, row - lat + HALO) * lon + column
    pair = 2 * HALO
    beside = jnp.where(west, column + HALO, column - lon + HALO)
    tall = lat * pair
    side = jnp.where(west, 0, sides - 1)
    column_index = 2 * strip + side * tall + row * pair + beside
    corner_row = jnp.where(above, row + HALO, row - lat)
    corner = jnp.where(above, 0, 1) * sides + side
    corner_index = 2 * strip + sides * tall + corner * lon + corner_row * pair + beside
    halo = jnp.where(
        outside_column == 0,
        jnp.where(outside_row == 0, -1, row_index),
        jnp.where(outside_row == 0, column_index, corner_index),
    )
    return jnp.where(inside, row, -1), jnp.where(inside, column, -1), halo


def kernel(
    x_hbm, w1_hbm, w2_hbm, e1_hbm, e2_hbm, b1_hbm, gain_hbm, eb1_hbm, mgain_hbm, mbias_hbm,
    mesh_hbm, edge_hbm, senders_hbm, receivers_hbm, count_hbm,
    stage, mean_ref,
    x_ref, wide, xw, w1_in, w1_wide, w1, w2_in, w2, e1_ref, e2_in, e2_ref, vec_ref, cols,
    senders_ref, receivers_ref, count_ref, near_ref, place_ref, cmask, gathered, out_wide, sender_ref, half_ref,
    cols_send, rows_recv, rows_all, cols_recv, corner_recv,
    assigned, nodes_all, totals, sent, parts, degree_ref,
    x_sem, in_sem, halo_send, halo_recv, z_send, z_recv,
):
    tiles, channels, rows, lon = x_ref.shape
    lat = tiles * rows
    padded = w1.shape[1]
    latent, share = assigned.shape
    shard, nodes = parts.shape[1:]
    slots = receivers_ref.shape[1]
    layers = slots // share
    sides = cols_recv.shape[0]
    groups = rows // GROUP
    me = lax.axis_index("gz")
    mine = pl.ds(pl.multiple_of(me * shard, shard), shard)
    own_edges = pl.ds(pl.multiple_of(me * share, share), share)

    steps = (1,) if sides == 1 else (-1, 1)
    around = [(1, 0, 0), (-1, 0, 0)] + [(0, dy, 0) for dy in steps]
    around += [(dx, dy, 0) for dx in (1, -1) for dy in steps]
    around += [(0, 0, k) for k in range(1, layers)]
    barrier = pltpu.get_barrier_semaphore()
    for offset in around:
        pl.semaphore_signal(barrier, inc=1, device_id=partner(*offset), device_id_type=MESH)
    local = [
        (w1_hbm, w1_in), (w2_hbm, w2_in), (senders_hbm, senders_ref), (receivers_hbm, receivers_ref),
        (count_hbm, count_ref), (e1_hbm, e1_ref), (e2_hbm, e2_in),
        (mesh_hbm, nodes_all.at[mine, :]), (edge_hbm.at[:, own_edges], assigned.at[mine, :]),
    ]
    local += [
        (ref, vec_ref.at[pl.ds(i, 1), :])
        for i, ref in enumerate((b1_hbm, gain_hbm, eb1_hbm, mgain_hbm, mbias_hbm))
    ]
    local = [pltpu.make_async_copy(a, b, in_sem.at[i]) for i, (a, b) in enumerate(local)]
    loads = [
        pltpu.make_async_copy(x_hbm.at[:, pl.ds(t * rows, rows), :], x_ref.at[t], x_sem.at[t])
        for t in range(tiles)
    ]
    for load in loads + local:
        load.start()
    pl.semaphore_wait(barrier, len(around))

    spread = []
    for k in range(1, layers):
        peer = lax.rem(me + k, layers)
        theirs = pl.ds(pl.multiple_of(peer * share, share), share)
        spread.append(
            remote(mesh_hbm, nodes_all.at[mine, :], z_send.at[1, k], z_recv.at[1, k], (0, 0, k))
        )
        spread.append(
            remote(edge_hbm.at[:, theirs], assigned.at[mine, :], z_send.at[0, k], z_recv.at[0, k], (0, 0, k))
        )
    halo = [
        remote(x_hbm.at[:, pl.ds(lat - HALO, HALO), :], rows_recv.at[0], halo_send.at[0], halo_recv.at[0], (1, 0, 0)),
        remote(x_hbm.at[:, pl.ds(0, HALO), :], rows_recv.at[1], halo_send.at[1], halo_recv.at[1], (-1, 0, 0)),
    ]
    for copy in spread + halo:
        copy.start()

    wide[...] = jnp.zeros_like(wide)

    def relay(source, slot, height):
        wide[slot, pl.ds(0, channels * height), :] = source.astype(F32).reshape(channels * height, lon)

        def row(j):
            return wide[slot, pl.ds(j, padded, stride=height), :].astype(BF16)

        return row

    lanes = lax.broadcasted_iota(jnp.int32, (padded, lon), 1) // (2 * HALO)

    def widen(t, carry):
        pltpu.make_async_copy(
            x_hbm.at[:, pl.ds(t * rows, rows), :], x_ref.at[t], x_sem.at[t]
        ).wait()
        row_of = relay(x_ref[t], 0, rows)
        for half in range(rows // HALO):
            beside = jnp.zeros((padded, lon), F32)
            for j in range(HALO):
                r = half * HALO + j
                value = wide[0, pl.ds(r, padded, stride=rows), :]
                xw[t * groups + r // GROUP, :, (r % GROUP) * lon : (r % GROUP + 1) * lon] = value.astype(BF16)
                turn = (2 * j * HALO + HALO) % lon
                beside = jnp.where(lanes == j, pltpu.roll(value, turn, 1), beside)
            cols_send[t * (rows // HALO) + half] = beside.astype(BF16)
        return carry

    lax.fori_loop(0, tiles, widen, 0)
    for i, dy in enumerate(steps):
        slot = sides - 1 - i
        halo.append(
            remote(cols_send, cols_recv.at[slot], halo_send.at[2 + i], halo_recv.at[2 + i], (0, dy, 0))
        )
        for n, dx in enumerate((1, -1)):
            block = cols_send.at[lat // HALO - 1 if dx > 0 else 0]
            at = 4 + 2 * n + i
            halo.append(
                remote(block, corner_recv.at[n, slot], halo_send.at[at], halo_recv.at[at], (dx, dy, 0))
            )
    for copy in halo[2:]:
        copy.start()

    for copy in local:
        copy.wait()
    w1_wide[...] = jnp.zeros_like(w1_wide)
    w1_wide[:channels, :] = w1_in[...].astype(F32) * 0.5
    w1[...] = w1_wide[...].T[:, :padded].astype(BF16)
    cols[...] = vec_ref[...].T
    average = jnp.mean(w2_in[...].astype(F32), axis=0, keepdims=True)
    for k in range(layers):
        block = pl.ds(pl.multiple_of(lax.rem(me + k, layers) * shard, shard), shard)
        w2[pl.ds(k * shard, shard), :] = (w2_in[block, :].astype(F32) - average).astype(BF16)
    e2_wide = e2_in[...].astype(F32)
    e2_ref[...] = (e2_wide - jnp.mean(e2_wide, axis=0, keepdims=True)).astype(BF16)
    tile = lax.axis_index("gx") * lax.axis_size("gy") + lax.axis_index("gy")
    slot_ids = lax.broadcasted_iota(jnp.int32, (1, slots), 1)
    near_ref[...] = jnp.where(slot_ids < count_ref[...], receivers_ref[...] - tile * nodes, -1)
    own_row, own_column, own_halo = locate(senders_ref[:, own_edges], lat, lon, sides)
    place_ref[0:1, :] = own_row
    place_ref[1:2, :] = own_halo
    place_ref[2:3, :] = near_ref[:, own_edges]
    cmask[...] = onehot_of(own_column, 0, lon)
    gathered[...] = jnp.zeros_like(gathered)
    b1 = cols[:, 0:1] * 0.5

    def pick_rows(first, count):
        picks = []
        for r in range(count):
            here = jnp.where(place_ref[0:1, :] == first + r, 1.0, 0.0)
            here = jnp.broadcast_to(here, (16, share)).astype(BF16)
            picks.append((cmask[...].reshape(lon // 16, 16, share) * here[None]).reshape(lon, share))
        return jnp.concatenate(picks, axis=0)

    def gather(g, carry):
        gathered[...] += jnp.dot(xw[g], pick_rows(g * GROUP, GROUP), preferred_element_type=F32)
        return carry

    lax.fori_loop(0, tiles * groups, gather, 0)

    def first_layer(g):
        half = jnp.dot(w1[...], xw[g], preferred_element_type=F32) + b1
        return half_silu(half).astype(BF16)

    def embed(t, carry):
        own_gain = cols[mine, 1:2]
        hidden = first_layer(t * groups)
        for group in range(groups):
            pre = jnp.dot(w2[...], hidden, preferred_element_type=F32)
            if group + 1 < groups:
                hidden = first_layer(t * groups + group + 1)
            own = pre[:shard, :] * inverse_spread(pre) * own_gain
            for r in range(GROUP):
                out_wide[pl.ds(group * GROUP + r, shard, stride=rows), :] = own[
                    :, r * lon : (r + 1) * lon
                ]
        stage[t] = out_wide[...].reshape(shard, rows, lon).astype(BF16)
        return carry

    lax.fori_loop(0, EARLY, embed, 0)

    last = (((1,), (1,)), ((), ()))
    degree = jnp.zeros((8, nodes), F32)
    for start in range(0, slots, share):
        chunk = onehot_of(near_ref[:, start : start + share], 0, nodes)
        ones = jnp.ones((8, share), BF16)
        degree = degree + lax.dot_general(ones, chunk, last, preferred_element_type=F32)
    degree_ref[...] = jnp.maximum(degree, 1.0)

    for copy in halo:
        copy.wait()
    for i in range(2):
        row_of = relay(rows_recv[i], 0, HALO)
        for j in range(HALO):
            rows_all[i, :, j * lon : (j + 1) * lon] = row_of(j)
    picked = gathered[...]
    pieces = [rows_all[0], rows_all[1]]
    for side in range(sides):
        pieces.append(jnp.concatenate([cols_recv[side, b] for b in range(lat // HALO)], axis=1))
    pieces.append(jnp.concatenate([corner_recv[n, side] for n in range(2) for side in range(sides)], axis=1))
    first = 0
    for piece in pieces:
        pick = onehot_of(place_ref[1:2, :], first, piece.shape[1])
        picked = picked + jnp.dot(piece, pick, preferred_element_type=F32)
        first += piece.shape[1]
    half = jnp.dot(w1[...], picked.astype(BF16), preferred_element_type=F32) + b1
    hidden = half_silu(half).astype(BF16)
    pre = jnp.dot(w2[...], hidden, preferred_element_type=F32)
    scale = inverse_spread(pre)
    for k in range(layers):
        block = pl.ds(pl.multiple_of(lax.rem(me + k, layers) * shard, shard), shard)
        part = pre[k * shard : (k + 1) * shard, :] * scale * cols[block, 1:2]
        sender_ref[block, :] = part.astype(BF16)
    half_ref[...] = jnp.dot(e1_ref[:, latent : 2 * latent], sender_ref[...], preferred_element_type=F32)

    for copy in spread:
        copy.wait()
    onehot = onehot_of(place_ref[2:3, :], 0, nodes)
    mesh_cols = jnp.dot(nodes_all[...], onehot, preferred_element_type=F32).astype(BF16)
    half = half_ref[...] + jnp.dot(e1_ref[:, :latent], assigned[...], preferred_element_type=F32)
    half = half + jnp.dot(e1_ref[:, 2 * latent :], mesh_cols, preferred_element_type=F32)
    hidden = half_silu((half + cols[:, 2:3]) * 0.5).astype(BF16)
    second = jnp.dot(e2_ref[...], hidden, preferred_element_type=F32)
    message = (
        assigned[...].astype(F32) + second * inverse_spread(second) * cols[:, 3:4] + cols[:, 4:5]
    ).astype(BF16)
    totals[...] = lax.dot_general(message, onehot, last, preferred_element_type=F32)
    sent[...] = totals[...].astype(BF16)
    exchange = []
    for k in range(1, layers):
        peer = lax.rem(me + k, layers)
        theirs = pl.ds(pl.multiple_of(peer * shard, shard), shard)
        exchange.append(
            remote(sent.at[theirs, :], parts.at[k], z_send.at[2, k], z_recv.at[2, k], (0, 0, k))
        )
    for copy in exchange:
        copy.start()

    lax.fori_loop(EARLY, tiles, embed, 0)

    for copy in exchange:
        copy.wait()
    total = totals[mine, :]
    for k in range(1, layers):
        total = total + parts[k].astype(F32)
    mean_ref[...] = (nodes_all[mine, :].astype(F32) + total / degree_ref[0:1, :]).astype(BF16)


def finish(stage, mesh_ref, grid_out, mesh_out, sem):
    tiles, _, rows, _ = stage.shape
    copies = [
        pltpu.make_async_copy(stage.at[t], grid_out.at[:, pl.ds(t * rows, rows), :], sem.at[t])
        for t in range(tiles)
    ]
    copies.append(pltpu.make_async_copy(mesh_ref, mesh_out, sem.at[tiles]))
    for copy in copies:
        copy.start()
    for copy in copies:
        copy.wait()


def on_device(
    grid_inputs,
    embed_w1,
    embed_b1,
    embed_w2,
    embed_gain,
    edge_w1,
    edge_b1,
    edge_w2,
    message_gain,
    message_bias,
    mesh_latent,
    edge_latent,
    senders,
    receivers,
    edge_counts,
):
    latent = embed_w2.shape[0]
    channels, lat, lon = grid_inputs.shape
    shard = mesh_latent.shape[0]
    nodes = mesh_latent.shape[3]
    slots = edge_latent.shape[3]
    layers = lax.axis_size("gz")
    sides = 1 if lax.axis_size("gy") == 2 else 2
    share = slots // layers
    padded = -(-channels // 16) * 16
    tiles = lat // ROWS
    I32 = jnp.int32

    vmem = pl.BlockSpec(memory_space=pltpu.VMEM)
    hbm = pl.BlockSpec(memory_space=pltpu.HBM)
    scratch = [
        ((tiles, channels, ROWS, lon), BF16),
        ((1, padded * ROWS, lon), F32),
        ((lat // GROUP, padded, GROUP * lon), BF16),
        ((channels, latent), BF16),
        ((-(-padded // 128) * 128, latent), F32),
        ((latent, padded), BF16),
        (embed_w2.shape, BF16),
        (embed_w2.shape, BF16),
        (edge_w1.shape, BF16),
        (edge_w2.shape, BF16),
        (edge_w2.shape, BF16),
        ((8, latent), F32),
        ((latent, 8), F32),
        ((1, slots), I32),
        ((1, slots), I32),
        ((1, 1), I32),
        ((1, slots), I32),
        ((8, share), I32),
        ((lon, share), BF16),
        ((padded, share), F32),
        ((shard * ROWS, lon), F32),
        ((latent, share), BF16),
        ((latent, share), F32),
        ((lat // HALO, padded, lon), BF16),
        ((2, channels, HALO, lon), BF16),
        ((2, padded, HALO * lon), BF16),
        ((sides, lat // HALO, padded, lon), BF16),
        ((2, sides, padded, lon), BF16),
        ((latent, share), BF16),
        ((latent, nodes), BF16),
        ((latent, nodes), F32),
        ((latent, nodes), BF16),
        ((layers, shard, nodes), BF16),
        ((8, nodes), F32),
    ]
    sems = [(tiles,), (14,), (8,), (8,), (3, layers), (3, layers)]
    line = lambda v: v.reshape(1, v.size)
    stage, mean = pl.pallas_call(
        kernel,
        in_specs=[hbm] * 15,
        out_specs=[vmem, vmem],
        out_shape=[
            pltpu.VMEM((tiles, shard, ROWS, lon), BF16),
            pltpu.VMEM((shard, nodes), BF16),
        ],
        scratch_shapes=[pltpu.VMEM(s, d) for s, d in scratch]
        + [pltpu.SemaphoreType.DMA(s) for s in sems],
        compiler_params=pltpu.CompilerParams(
            collective_id=0, has_side_effects=True, vmem_limit_bytes=64_860_000
        ),
    )(
        grid_inputs, embed_w1.T, embed_w2, edge_w1, edge_w2,
        line(embed_b1), line(embed_gain), line(edge_b1), line(message_gain), line(message_bias),
        mesh_latent[:, 0, 0, :], edge_latent[:, 0, 0, :], line(senders), line(receivers), edge_counts,
    )
    grid_out, mesh_out = pl.pallas_call(
        finish,
        in_specs=[vmem, vmem],
        out_specs=[hbm, hbm],
        out_shape=[
            jax.ShapeDtypeStruct((shard, lat, lon), BF16),
            jax.ShapeDtypeStruct((shard, nodes), BF16),
        ],
        scratch_shapes=[pltpu.SemaphoreType.DMA((tiles + 1,))],
        compiler_params=pltpu.CompilerParams(vmem_limit_bytes=1024 * 1024),
    )(
        pltpu.with_memory_space_constraint(stage, pltpu.VMEM),
        pltpu.with_memory_space_constraint(mean, pltpu.VMEM),
    )
    return (mesh_out.reshape(shard, 1, 1, nodes), grid_out)


def solution(mesh):
    return jax.shard_map(
        on_device,
        mesh=mesh,
        in_specs=(
            P(None, "gx", "gy"),
            P(),
            P(),
            P(),
            P(),
            P(),
            P(),
            P(),
            P(),
            P(),
            P("gz", "gx", "gy", None),
            P("gz", "gx", "gy", None),
            P("gx", "gy", None),
            P("gx", "gy", None),
            P("gx", "gy"),
        ),
        out_specs=(P("gz", "gx", "gy", None), P("gz", "gx", "gy")),
        check_vma=False,
    )
```

```python
import jax
import jax.numpy as jnp
from jax import lax
from jax.experimental import pallas as pl
from jax.experimental.pallas import tpu as pltpu
from jax.sharding import PartitionSpec as P

HALO = 8
ROWS = 16
GROUP = 4
EARLY = 2
PARTS = 2
REACH = 2

epsilon = 1e-05
F32 = jnp.float32
BF16 = jnp.bfloat16
MESH = pl.DeviceIdType.MESH


def half_silu(half):
    return half + half * jnp.tanh(half)


def inverse_spread(values):
    return lax.rsqrt(jnp.mean(values * values, axis=0, keepdims=True) + epsilon)


def onehot_of(index_row, first, count):
    ids = lax.broadcasted_iota(jnp.int32, (count, index_row.shape[1]), 0)
    return jnp.where(ids == index_row - first, 1.0, 0.0).astype(BF16)


def partner(dx, dy, dz):
    ids = {}
    for axis, step in (("gx", dx), ("gy", dy), ("gz", dz)):
        size = lax.axis_size(axis)
        ids[axis] = lax.rem(lax.axis_index(axis) + (step + size), size)
    return ids


def remote(source, target, send_sem, recv_sem, offset):
    return pltpu.make_async_remote_copy(
        src_ref=source, dst_ref=target, send_sem=send_sem, recv_sem=recv_sem,
        device_id=partner(*offset), device_id_type=MESH,
    )


def split(values, size):
    if size & (size - 1) == 0:
        return lax.shift_right_logical(values, size.bit_length() - 1), values & (size - 1)
    return values // size, values % size


def locate(send, lat, lon, sides):
    band = lax.axis_index("gx")
    sector = lax.axis_index("gy")
    lon_total = lon * lax.axis_size("gy")
    row, column = split(send, lon_total)
    row = row - band * lat
    column = split(column - sector * lon + (HALO + lon_total), lon_total)[1] - HALO
    above, below = row < 0, row >= lat
    west, east = column < 0, column >= lon
    outside_row = jnp.where(above, 1, jnp.where(below, 1, 0))
    outside_column = jnp.where(west, 1, jnp.where(east, 1, 0))
    tall = lat // HALO
    side = jnp.where(west, 0, sides - 1)
    beside = jnp.where(west, column + HALO, column - lon + HALO)
    row_block = lat + jnp.where(above, row + HALO, row - lat + HALO)
    column_block = lat + 2 * HALO + side * tall + lax.shift_right_arithmetic(row, HALO.bit_length() - 1)
    corner_block = lat + 2 * HALO + sides * tall + jnp.where(above, 0, 1) * sides + side
    block = jnp.where(
        outside_column == 0,
        jnp.where(outside_row == 0, row, row_block),
        jnp.where(outside_row == 0, column_block, corner_block),
    )
    lane = jnp.where(outside_column == 0, column, (row & (HALO - 1)) * (2 * HALO) + beside)
    return block, lane


def kernel(
    x_hbm, w1_hbm, w2_hbm, e1_hbm, e2_hbm, b1_hbm, gain_hbm, eb1_hbm, mgain_hbm, mbias_hbm,
    mesh_hbm, edge_hbm, senders_hbm, receivers_hbm, count_hbm,
    stage, mean_ref,
    x_ref, wide, xw, w1_in, w1_wide, w1, w2_in, w2, e1_ref, e2_in, e2_ref, vec_ref, cols,
    senders_ref, receivers_ref, count_ref, near_ref, place_ref, cmask, out_wide, sender_ref, half_ref,
    cols_send, rows_recv, rows_all, cols_recv, corner_recv,
    assigned, nodes_all, totals, sent, parts, degree_ref,
    x_sem, in_sem, halo_send, halo_recv, col_send, col_recv, z_send, z_recv, n_send, n_recv,
):
    tiles, channels, rows, lon = x_ref.shape
    lat = tiles * rows
    padded = w1.shape[1]
    latent, share = assigned.shape
    shard, nodes = parts.shape[1:]
    slots = receivers_ref.shape[1]
    layers = slots // share
    sides = cols_recv.shape[0]
    groups = rows // GROUP
    me = lax.axis_index("gz")
    mine = pl.ds(pl.multiple_of(me * shard, shard), shard)
    own_edges = pl.ds(pl.multiple_of(me * share, share), share)

    steps = (1,) if sides == 1 else (-1, 1)
    bands = lax.axis_size("gx")
    band = lax.axis_index("gx")

    def inside(dx):
        return jnp.logical_and(band + dx >= 0, band + dx < bands)

    def when_inside(dx, action):
        @pl.when(inside(dx))
        def _():
            action()

    barrier = pltpu.get_barrier_semaphore()

    def greet(offset):
        pl.semaphore_signal(barrier, inc=1, device_id=partner(*offset), device_id_type=MESH)

    peers = [(0, 0, k) for k in range(1, layers)] + [(0, dy, 0) for dy in steps]
    for offset in peers:
        greet(offset)
    across = [(0,)] + [(dy,) for dy in steps]
    for dx in (1, -1):
        when_inside(dx, lambda: [greet((dx, *dy, 0)) for dy in across])
    greetings = len(peers) + len(across) * (2 - (band == 0).astype(jnp.int32) - (band == bands - 1).astype(jnp.int32))
    local = [
        (w1_hbm, w1_in), (w2_hbm, w2_in), (senders_hbm, senders_ref), (receivers_hbm, receivers_ref),
        (count_hbm, count_ref), (e1_hbm, e1_ref), (e2_hbm, e2_in),
        (mesh_hbm, nodes_all.at[mine, :]), (edge_hbm.at[:, own_edges], assigned.at[mine, :]),
    ]
    local += [
        (ref, vec_ref.at[pl.ds(i, 1), :])
        for i, ref in enumerate((b1_hbm, gain_hbm, eb1_hbm, mgain_hbm, mbias_hbm))
    ]
    local = [pltpu.make_async_copy(a, b, in_sem.at[i]) for i, (a, b) in enumerate(local)]
    loads = [
        pltpu.make_async_copy(x_hbm.at[:, pl.ds(t * rows, rows), :], x_ref.at[t], x_sem.at[t])
        for t in range(tiles)
    ]
    for load in loads + local:
        load.start()
    pl.semaphore_wait(barrier, greetings)

    def along(step):
        return jnp.logical_and(me + step >= 0, me + step < layers)

    def nodes_to(block, step, source):
        at = pl.ds(pl.multiple_of(block * shard, shard), shard)
        return pltpu.make_async_remote_copy(
            src_ref=source, dst_ref=nodes_all.at[at, :],
            send_sem=n_send.at[block, step + layers - 1], recv_sem=n_recv.at[block],
            device_id={"gz": jnp.clip(me + step, 0, layers - 1)}, device_id_type=MESH,
        )

    hops = [step for far in range(1, min(REACH, layers - 1) + 1) for step in (far, -far)]
    passed = [(far, way) for far in range(REACH + 1, layers) for way in (1, -1)]

    def every_hop(action):
        for step in hops:
            @pl.when(along(step))
            def _():
                action(nodes_to(me, step, mesh_hbm))

    def every_pass(action):
        for far, way in passed:
            block = me - REACH * way
            step = (far - REACH) * way

            @pl.when(jnp.logical_and(along(-REACH * way), along(step)))
            def _():
                at = pl.ds(pl.multiple_of(block * shard, shard), shard)
                action(nodes_to(block, step, nodes_all.at[at, :]), far == REACH + 1)

    def pass_nodes(copy, first):
        if first:
            copy.wait_recv()
        copy.start()

    def receive_nodes():
        for far in range(1, layers):
            for way in (1, -1):
                early = jnp.logical_and(far == REACH, along(way)) if passed else False

                @pl.when(jnp.logical_and(along(-far * way), jnp.logical_not(early)))
                def _():
                    nodes_to(me - far * way, way, mesh_hbm).wait_recv()

    every_hop(lambda copy: copy.start())

    part = share // PARTS
    spread = []
    for c in range(PARTS):
        for k in range(1, layers):
            peer = lax.rem(me + k, layers)
            theirs = pl.ds(pl.multiple_of(peer * share + c * part, part), part)
            spread.append(
                remote(
                    edge_hbm.at[:, theirs], assigned.at[mine, pl.ds(c * part, part)],
                    z_send.at[c, k], z_recv.at[c, k], (0, 0, k),
                )
            )
    row_halo = [
        remote(x_hbm.at[:, pl.ds(lat - HALO, HALO), :], rows_recv.at[0], halo_send.at[0], halo_recv.at[0], (1, 0, 0)),
        remote(x_hbm.at[:, pl.ds(0, HALO), :], rows_recv.at[1], halo_send.at[1], halo_recv.at[1], (-1, 0, 0)),
    ]
    for copy in spread[: layers - 1]:
        copy.start()
    for copy, dx in zip(row_halo, (1, -1)):
        when_inside(dx, copy.start)
    corners = []
    for i, dy in enumerate(steps):
        slot = sides - 1 - i
        for n, dx in enumerate((1, -1)):
            block = cols_send.at[lat // HALO - 1 if dx > 0 else 0]
            at = 2 + 2 * n + i
            corners.append(
                (n, remote(block, corner_recv.at[n, slot], halo_send.at[at], halo_recv.at[at], (dx, dy, 0)))
            )

    def fill(n):
        rows_recv[n] = jnp.zeros(rows_recv.shape[1:], BF16)
        corner_recv[n] = jnp.zeros(corner_recv.shape[1:], BF16)

    pl.when(band == 0)(lambda: fill(0))
    pl.when(band == bands - 1)(lambda: fill(1))

    def strips(t, i):
        blocks = pl.ds(t * (rows // HALO), rows // HALO)
        return remote(
            cols_send.at[blocks], cols_recv.at[sides - 1 - i, blocks],
            col_send.at[i, t], col_recv.at[i, t], (0, steps[i], 0),
        )

    def relay(source, slot, height):
        wide[slot, pl.ds(0, channels * height), :] = source.astype(F32).reshape(channels * height, lon)
        wide[slot, pl.ds(channels * height, (padded - channels) * height), :] = jnp.zeros(
            ((padded - channels) * height, lon), F32
        )

        def row(j):
            return wide[slot, pl.ds(j, padded, stride=height), :].astype(BF16)

        return row

    lanes = lax.broadcasted_iota(jnp.int32, (padded, lon), 1) // (2 * HALO)

    def widen(t, carry):
        pltpu.make_async_copy(
            x_hbm.at[:, pl.ds(t * rows, rows), :], x_ref.at[t], x_sem.at[t]
        ).wait()

        @pl.when(t > 0)
        def _():
            for i in range(len(steps)):
                strips(t - 1, i).start()

        relay(x_ref[t], 0, rows)
        for half in range(rows // HALO):
            beside = jnp.zeros((padded, lon), F32)
            for j in range(HALO):
                r = half * HALO + j
                value = wide[0, pl.ds(r, padded, stride=rows), :]
                xw[t * groups + r // GROUP, :, (r % GROUP) * lon : (r % GROUP + 1) * lon] = value.astype(BF16)
                turn = (2 * j * HALO + HALO) % lon
                beside = jnp.where(lanes == j, pltpu.roll(value, turn, 1), beside)
            cols_send[t * (rows // HALO) + half] = beside.astype(BF16)
        return carry

    lax.fori_loop(0, tiles, widen, 0)
    for i in range(len(steps)):
        strips(tiles - 1, i).start()
    for n, copy in corners:
        when_inside(1 - 2 * n, copy.start)
    for copy in spread[layers - 1 :]:
        copy.start()

    for copy in local:
        copy.wait()
    w1_wide[...] = jnp.zeros_like(w1_wide)
    w1_wide[:channels, :] = w1_in[...].astype(F32) * 0.5
    w1[...] = w1_wide[...].T[:, :padded].astype(BF16)
    cols[...] = vec_ref[...].T
    average = jnp.mean(w2_in[...].astype(F32), axis=0, keepdims=True)
    for k in range(layers):
        block = pl.ds(pl.multiple_of(lax.rem(me + k, layers) * shard, shard), shard)
        w2[pl.ds(k * shard, shard), :] = (w2_in[block, :].astype(F32) - average).astype(BF16)
    e2_wide = e2_in[...].astype(F32)
    e2_ref[...] = (e2_wide - jnp.mean(e2_wide, axis=0, keepdims=True)).astype(BF16)
    tile = lax.axis_index("gx") * lax.axis_size("gy") + lax.axis_index("gy")
    slot_ids = lax.broadcasted_iota(jnp.int32, (1, slots), 1)
    near_ref[...] = jnp.where(slot_ids < count_ref[...], receivers_ref[...] - tile * nodes, -1)
    block, lane = locate(senders_ref[:, own_edges], lat, lon, sides)
    place_ref[0:1, :] = block
    place_ref[2:3, :] = near_ref[:, own_edges]
    cmask[...] = onehot_of(lane, 0, lon)
    b1 = cols[:, 0:1] * 0.5

    def pick_rows(first, count):
        picks = []
        for r in range(count):
            here = jnp.where(place_ref[0:1, :] == first + r, 1.0, 0.0)
            here = jnp.broadcast_to(here, (16, share)).astype(BF16)
            picks.append((cmask[...].reshape(lon // 16, 16, share) * here[None]).reshape(lon, share))
        return jnp.concatenate(picks, axis=0)

    def first_layer(g):
        half = jnp.dot(w1[...], xw[g], preferred_element_type=F32) + b1
        return half_silu(half).astype(BF16)

    own_gain = cols[mine, 1:2]

    def embed(start, stop):
        hidden = first_layer(start * groups)
        for g in range(start * groups, stop * groups):
            t, group = g // groups, g % groups
            pre = jnp.dot(w2[...], hidden, preferred_element_type=F32)
            if g + 1 < stop * groups:
                hidden = first_layer(g + 1)
            own = pre[:shard, :] * inverse_spread(pre) * own_gain
            for r in range(GROUP):
                out_wide[t, pl.ds(group * GROUP + r, shard, stride=rows), :] = own[
                    :, r * lon : (r + 1) * lon
                ]
            if group + 1 == groups:
                stage[t] = out_wide[t].reshape(shard, rows, lon).astype(BF16)

    picked = jnp.zeros((padded, share), F32)
    for t in range(tiles):
        cells = jnp.concatenate([xw[t * groups + g] for g in range(groups)], axis=1)
        picked = picked + jnp.dot(cells, pick_rows(t * rows, rows), preferred_element_type=F32)
    half_ref[0:padded, :] = picked
    last = (((1,), (1,)), ((), ()))
    degree = jnp.zeros((8, nodes), F32)
    for start in range(0, slots, share):
        chunk = onehot_of(near_ref[:, start : start + share], 0, nodes)
        ones = jnp.ones((8, share), BF16)
        degree = degree + lax.dot_general(ones, chunk, last, preferred_element_type=F32)
    degree_ref[...] = jnp.maximum(degree, 1.0)
    embed(0, 1)

    every_pass(pass_nodes)
    for n, copy in enumerate(row_halo):
        when_inside(1 - 2 * n, copy.wait_send)
        when_inside(2 * n - 1, copy.wait_recv)
    for i in range(2):
        row_of = relay(rows_recv[i], 0, HALO)
        for j in range(HALO):
            rows_all[i, :, j * lon : (j + 1) * lon] = row_of(j)
    cells = jnp.concatenate([rows_all[0], rows_all[1]], axis=1)
    half_ref[0:padded, :] += jnp.dot(cells, pick_rows(lat, 2 * HALO), preferred_element_type=F32)
    embed(1, EARLY)

    for t in range(tiles):
        for i in range(len(steps)):
            strips(t, i).wait()
    for n, copy in corners:
        when_inside(1 - 2 * n, copy.wait_send)
        when_inside(2 * n - 1, copy.wait_recv)
    pieces = [cols_recv[side, b] for side in range(sides) for b in range(lat // HALO)]
    pieces += [corner_recv[n, side] for n in range(2) for side in range(sides)]
    cells = jnp.concatenate(pieces, axis=1)
    picked = half_ref[0:padded, :] + jnp.dot(
        cells, pick_rows(lat + 2 * HALO, cells.shape[1] // lon), preferred_element_type=F32
    )
    half = jnp.dot(w1[...], picked.astype(BF16), preferred_element_type=F32) + b1
    hidden = half_silu(half).astype(BF16)
    pre = jnp.dot(w2[...], hidden, preferred_element_type=F32)
    scale = inverse_spread(pre)
    for k in range(layers):
        block = pl.ds(pl.multiple_of(lax.rem(me + k, layers) * shard, shard), shard)
        rows_k = pre[k * shard : (k + 1) * shard, :] * scale * cols[block, 1:2]
        sender_ref[block, :] = rows_k.astype(BF16)
    half_ref[...] = jnp.dot(e1_ref[:, latent : 2 * latent], sender_ref[...], preferred_element_type=F32)

    receive_nodes()
    onehot = onehot_of(place_ref[2:3, :], 0, nodes)
    mesh_cols = jnp.dot(nodes_all[...], onehot, preferred_element_type=F32).astype(BF16)
    half_ref[...] += jnp.dot(e1_ref[:, 2 * latent :], mesh_cols, preferred_element_type=F32) + cols[:, 2:3]

    for c in range(PARTS):
        for copy in spread[c * (layers - 1) : (c + 1) * (layers - 1)]:
            copy.wait()
        at = slice(c * part, (c + 1) * part)
        half = half_ref[:, at] + jnp.dot(e1_ref[:, :latent], assigned[:, at], preferred_element_type=F32)
        hidden = half_silu(half * 0.5).astype(BF16)
        second = jnp.dot(e2_ref[...], hidden, preferred_element_type=F32)
        message = (
            assigned[:, at].astype(F32) + second * inverse_spread(second) * cols[:, 3:4] + cols[:, 4:5]
        ).astype(BF16)
        onehot = onehot_of(place_ref[2:3, at], 0, nodes)
        sums = lax.dot_general(message, onehot, last, preferred_element_type=F32)
        totals[...] = sums if c == 0 else totals[...] + sums
    sent[...] = totals[...].astype(BF16)
    every_hop(lambda copy: copy.wait_send())
    every_pass(lambda copy, first: copy.wait_send())
    exchange = []
    for k in range(1, layers):
        peer = lax.rem(me + k, layers)
        theirs = pl.ds(pl.multiple_of(peer * shard, shard), shard)
        exchange.append(
            remote(sent.at[theirs, :], parts.at[k], z_send.at[PARTS, k], z_recv.at[PARTS, k], (0, 0, k))
        )
    for copy in exchange:
        copy.start()

    embed(EARLY, tiles)

    for copy in exchange:
        copy.wait()
    total = totals[mine, :]
    for k in range(1, layers):
        total = total + parts[k].astype(F32)
    mean_ref[...] = (nodes_all[mine, :].astype(F32) + total / degree_ref[0:1, :]).astype(BF16)


def finish(stage, mesh_ref, grid_out, mesh_out, sem):
    tiles, _, rows, _ = stage.shape
    copies = [
        pltpu.make_async_copy(stage.at[t], grid_out.at[:, pl.ds(t * rows, rows), :], sem.at[t])
        for t in range(tiles)
    ]
    copies.append(pltpu.make_async_copy(mesh_ref, mesh_out, sem.at[tiles]))
    for copy in copies:
        copy.start()
    for copy in copies:
        copy.wait()


def on_device(
    grid_inputs,
    embed_w1,
    embed_b1,
    embed_w2,
    embed_gain,
    edge_w1,
    edge_b1,
    edge_w2,
    message_gain,
    message_bias,
    mesh_latent,
    edge_latent,
    senders,
    receivers,
    edge_counts,
):
    latent = embed_w2.shape[0]
    channels, lat, lon = grid_inputs.shape
    shard = mesh_latent.shape[0]
    nodes = mesh_latent.shape[3]
    slots = edge_latent.shape[3]
    layers = lax.axis_size("gz")
    sides = 1 if lax.axis_size("gy") == 2 else 2
    share = slots // layers
    padded = -(-channels // 16) * 16
    tiles = lat // ROWS
    I32 = jnp.int32

    vmem = pl.BlockSpec(memory_space=pltpu.VMEM)
    hbm = pl.BlockSpec(memory_space=pltpu.HBM)
    scratch = [
        ((tiles, channels, ROWS, lon), BF16),
        ((1, padded * ROWS, lon), F32),
        ((lat // GROUP, padded, GROUP * lon), BF16),
        ((channels, latent), BF16),
        ((-(-padded // 128) * 128, latent), F32),
        ((latent, padded), BF16),
        (embed_w2.shape, BF16),
        (embed_w2.shape, BF16),
        (edge_w1.shape, BF16),
        (edge_w2.shape, BF16),
        (edge_w2.shape, BF16),
        ((8, latent), F32),
        ((latent, 8), F32),
        ((1, slots), I32),
        ((1, slots), I32),
        ((1, 1), I32),
        ((1, slots), I32),
        ((8, share), I32),
        ((lon, share), BF16),
        ((tiles, shard * ROWS, lon), F32),
        ((latent, share), BF16),
        ((latent, share), F32),
        ((lat // HALO, padded, lon), BF16),
        ((2, channels, HALO, lon), BF16),
        ((2, padded, HALO * lon), BF16),
        ((sides, lat // HALO, padded, lon), BF16),
        ((2, sides, padded, lon), BF16),
        ((latent, share), BF16),
        ((latent, nodes), BF16),
        ((latent, nodes), F32),
        ((latent, nodes), BF16),
        ((layers, shard, nodes), BF16),
        ((8, nodes), F32),
    ]
    sems = [(tiles,), (14,), (8,), (8,), (sides, tiles), (sides, tiles), (PARTS + 1, layers), (PARTS + 1, layers), (layers, 2 * layers - 1), (layers,)]
    line = lambda v: v.reshape(1, v.size)
    stage, mean = pl.pallas_call(
        kernel,
        in_specs=[hbm] * 15,
        out_specs=[vmem, vmem],
        out_shape=[
            pltpu.VMEM((tiles, shard, ROWS, lon), BF16),
            pltpu.VMEM((shard, nodes), BF16),
        ],
        scratch_shapes=[pltpu.VMEM(s, d) for s, d in scratch]
        + [pltpu.SemaphoreType.DMA(s) for s in sems],
        compiler_params=pltpu.CompilerParams(
            collective_id=0, has_side_effects=True, vmem_limit_bytes=64_860_000
        ),
    )(
        grid_inputs, embed_w1.T, embed_w2, edge_w1, edge_w2,
        line(embed_b1), line(embed_gain), line(edge_b1), line(message_gain), line(message_bias),
        mesh_latent[:, 0, 0, :], edge_latent[:, 0, 0, :], line(senders), line(receivers), edge_counts,
    )
    grid_out, mesh_out = pl.pallas_call(
        finish,
        in_specs=[vmem, vmem],
        out_specs=[hbm, hbm],
        out_shape=[
            jax.ShapeDtypeStruct((shard, lat, lon), BF16),
            jax.ShapeDtypeStruct((shard, nodes), BF16),
        ],
        scratch_shapes=[pltpu.SemaphoreType.DMA((tiles + 1,))],
        compiler_params=pltpu.CompilerParams(vmem_limit_bytes=1024 * 1024),
    )(
        pltpu.with_memory_space_constraint(stage, pltpu.VMEM),
        pltpu.with_memory_space_constraint(mean, pltpu.VMEM),
    )
    return (mesh_out.reshape(shard, 1, 1, nodes), grid_out)


def solution(mesh):
    return jax.shard_map(
        on_device,
        mesh=mesh,
        in_specs=(
            P(None, "gx", "gy"),
            P(),
            P(),
            P(),
            P(),
            P(),
            P(),
            P(),
            P(),
            P(),
            P("gz", "gx", "gy", None),
            P("gz", "gx", "gy", None),
            P("gx", "gy", None),
            P("gx", "gy", None),
            P("gx", "gy"),
        ),
        out_specs=(P("gz", "gx", "gy", None), P("gz", "gx", "gy")),
        check_vma=False,
    )
```

```python
import jax
import jax.numpy as jnp
from jax import lax
from jax.experimental import pallas as pl
from jax.experimental.pallas import tpu as pltpu
from jax.sharding import PartitionSpec as P

HALO = 8
ROWS = 16
GROUP = 4
EARLY = 2
PARTS = 2

epsilon = 1e-05
F32 = jnp.float32
BF16 = jnp.bfloat16
MESH = pl.DeviceIdType.MESH


def half_silu(half):
    return half + half * jnp.tanh(half)


def inverse_spread(values):
    return lax.rsqrt(jnp.mean(values * values, axis=0, keepdims=True) + epsilon)


def onehot_of(index_row, first, count):
    ids = lax.broadcasted_iota(jnp.int32, (count, index_row.shape[1]), 0)
    return jnp.where(ids == index_row - first, 1.0, 0.0).astype(BF16)


def partner(dx, dy, dz):
    ids = {}
    for axis, step in (("gx", dx), ("gy", dy), ("gz", dz)):
        size = lax.axis_size(axis)
        ids[axis] = lax.rem(lax.axis_index(axis) + (step + size), size)
    return ids


def remote(source, target, send_sem, recv_sem, offset):
    return pltpu.make_async_remote_copy(
        src_ref=source, dst_ref=target, send_sem=send_sem, recv_sem=recv_sem,
        device_id=partner(*offset), device_id_type=MESH,
    )


def split(values, size):
    if size & (size - 1) == 0:
        return lax.shift_right_logical(values, size.bit_length() - 1), values & (size - 1)
    return values // size, values % size


def locate(send, lat, lon, sides):
    band = lax.axis_index("gx")
    sector = lax.axis_index("gy")
    lon_total = lon * lax.axis_size("gy")
    row, column = split(send, lon_total)
    row = row - band * lat
    column = split(column - sector * lon + (HALO + lon_total), lon_total)[1] - HALO
    above, below = row < 0, row >= lat
    west, east = column < 0, column >= lon
    outside_row = jnp.where(above, 1, jnp.where(below, 1, 0))
    outside_column = jnp.where(west, 1, jnp.where(east, 1, 0))
    tall = lat // HALO
    side = jnp.where(west, 0, sides - 1)
    beside = jnp.where(west, column + HALO, column - lon + HALO)
    row_block = lat + jnp.where(above, row + HALO, row - lat + HALO)
    column_block = lat + 2 * HALO + side * tall + lax.shift_right_arithmetic(row, HALO.bit_length() - 1)
    corner_block = lat + 2 * HALO + sides * tall + jnp.where(above, 0, 1) * sides + side
    block = jnp.where(
        outside_column == 0,
        jnp.where(outside_row == 0, row, row_block),
        jnp.where(outside_row == 0, column_block, corner_block),
    )
    lane = jnp.where(outside_column == 0, column, (row & (HALO - 1)) * (2 * HALO) + beside)
    return block, lane


def kernel(
    x_hbm, w1_hbm, w2_hbm, e1_hbm, e2_hbm, b1_hbm, gain_hbm, eb1_hbm, mgain_hbm, mbias_hbm,
    mesh_hbm, edge_hbm, senders_hbm, receivers_hbm, count_hbm,
    stage, mean_ref,
    x_ref, wide, xw, w1_in, w1_wide, w1, w2_in, w2, e1_ref, e2_in, e2_ref, vec_ref, cols,
    senders_ref, receivers_ref, count_ref, near_ref, place_ref, cmask, out_wide, sender_ref, half_ref,
    cols_send, rows_recv, rows_all, cols_recv, corner_recv,
    assigned, nodes_all, totals, sent, parts, degree_ref,
    x_sem, in_sem, halo_send, halo_recv, col_send, col_recv, z_send, z_recv, n_send, n_recv,
):
    tiles, channels, rows, lon = x_ref.shape
    lat = tiles * rows
    padded = w1.shape[1]
    latent, share = assigned.shape
    shard, nodes = parts.shape[1:]
    slots = receivers_ref.shape[1]
    layers = slots // share
    sides = cols_recv.shape[0]
    groups = rows // GROUP
    me = lax.axis_index("gz")
    mine = pl.ds(pl.multiple_of(me * shard, shard), shard)
    own_edges = pl.ds(pl.multiple_of(me * share, share), share)

    steps = (1,) if sides == 1 else (-1, 1)
    bands = lax.axis_size("gx")
    band = lax.axis_index("gx")

    def inside(dx):
        return jnp.logical_and(band + dx >= 0, band + dx < bands)

    def when_inside(dx, action):
        @pl.when(inside(dx))
        def _():
            action()

    barrier = pltpu.get_barrier_semaphore()

    def greet(offset):
        pl.semaphore_signal(barrier, inc=1, device_id=partner(*offset), device_id_type=MESH)

    peers = [(0, 0, k) for k in range(1, layers)] + [(0, dy, 0) for dy in steps]
    for offset in peers:
        greet(offset)
    across = [(0,)] + [(dy,) for dy in steps]
    for dx in (1, -1):
        when_inside(dx, lambda: [greet((dx, *dy, 0)) for dy in across])
    greetings = len(peers) + len(across) * (2 - (band == 0).astype(jnp.int32) - (band == bands - 1).astype(jnp.int32))
    local = [
        (w1_hbm, w1_in), (w2_hbm, w2_in), (senders_hbm, senders_ref), (receivers_hbm, receivers_ref),
        (count_hbm, count_ref), (e1_hbm, e1_ref), (e2_hbm, e2_in),
        (mesh_hbm, nodes_all.at[mine, :]), (edge_hbm.at[:, own_edges], assigned.at[mine, :]),
    ]
    local += [
        (ref, vec_ref.at[pl.ds(i, 1), :])
        for i, ref in enumerate((b1_hbm, gain_hbm, eb1_hbm, mgain_hbm, mbias_hbm))
    ]
    local = [pltpu.make_async_copy(a, b, in_sem.at[i]) for i, (a, b) in enumerate(local)]
    loads = [
        pltpu.make_async_copy(x_hbm.at[:, pl.ds(t * rows, rows), :], x_ref.at[t], x_sem.at[t])
        for t in range(tiles)
    ]
    for load in loads + local:
        load.start()

    half_layers = layers // 2
    side = me // half_layers
    paired = layers == 4
    mate = me + 1 - 2 * lax.rem(me, 2)
    far_peers = [lax.rem((1 - side) * half_layers + j, layers) for j in range(half_layers)]
    near_peers = [side * half_layers + lax.rem(me + j, half_layers) for j in range(1, half_layers)]
    order = far_peers + near_peers
    if 2 * half_layers != layers:
        order = [lax.rem(me + k, layers) for k in range(1, layers)]

    def to_layer(source, target, send_sem, recv_sem, peer):
        return pltpu.make_async_remote_copy(
            src_ref=source, dst_ref=target, send_sem=send_sem, recv_sem=recv_sem,
            device_id={"gz": peer}, device_id_type=MESH,
        )

    def nodes_to(block, peer, slot, source):
        at = pl.ds(pl.multiple_of(block * shard, shard), shard)
        return to_layer(source, nodes_all.at[at, :], n_send.at[slot], n_recv.at[block], peer)

    if paired:
        direct = [nodes_to(me, peer, i, mesh_hbm) for i, peer in enumerate((2 - side, mate))]
    else:
        direct = [nodes_to(me, peer, i, mesh_hbm) for i, peer in enumerate(order)]
    is_hub = jnp.logical_and(me > 0, me < layers - 1)

    def passed():
        return [
            nodes_to(block, mate, 2 + i, nodes_all.at[pl.ds(pl.multiple_of(block * shard, shard), shard), :])
            for i, block in enumerate(far_peers)
        ]

    def pass_nodes():
        if paired:
            @pl.when(is_hub)
            def _():
                for copy in passed():
                    copy.wait_recv()
                    copy.start()

    def receive_nodes():
        for i, block in enumerate(near_peers if paired else order):
            nodes_to(block, mate, i, mesh_hbm).wait_recv()
        if paired:
            @pl.when(jnp.logical_not(is_hub))
            def _():
                for copy in passed():
                    copy.wait_recv()

    def sent_nodes():
        for copy in direct:
            copy.wait_send()
        if paired:
            @pl.when(is_hub)
            def _():
                for copy in passed():
                    copy.wait_send()

    part = share // PARTS
    spread = []
    for c in range(PARTS):
        for k, peer in enumerate(order):
            theirs = pl.ds(pl.multiple_of(peer * share + c * part, part), part)
            spread.append(
                to_layer(
                    edge_hbm.at[:, theirs], assigned.at[mine, pl.ds(c * part, part)],
                    z_send.at[c, k], z_recv.at[c, me], peer,
                )
            )
    row_halo = [
        remote(x_hbm.at[:, pl.ds(lat - HALO, HALO), :], rows_recv.at[0], halo_send.at[0], halo_recv.at[0], (1, 0, 0)),
        remote(x_hbm.at[:, pl.ds(0, HALO), :], rows_recv.at[1], halo_send.at[1], halo_recv.at[1], (-1, 0, 0)),
    ]
    corners = []
    for i, dy in enumerate(steps):
        slot = sides - 1 - i
        for n, dx in enumerate((1, -1)):
            block = cols_send.at[lat // HALO - 1 if dx > 0 else 0]
            at = 2 + 2 * n + i
            corners.append(
                (n, remote(block, corner_recv.at[n, slot], halo_send.at[at], halo_recv.at[at], (dx, dy, 0)))
            )

    def fill(n):
        rows_recv[n] = jnp.zeros(rows_recv.shape[1:], BF16)
        corner_recv[n] = jnp.zeros(corner_recv.shape[1:], BF16)

    pl.when(band == 0)(lambda: fill(0))
    pl.when(band == bands - 1)(lambda: fill(1))

    def strips(t, i):
        blocks = pl.ds(t * (rows // HALO), rows // HALO)
        return remote(
            cols_send.at[blocks], cols_recv.at[sides - 1 - i, blocks],
            col_send.at[i, t], col_recv.at[i, t], (0, steps[i], 0),
        )

    def send_strips(t):
        for i in range(len(steps)):
            strips(t, i).start()

    ahead = jnp.maximum(tiles - 1 - me, 0)

    def relay(source, slot, height):
        wide[slot, pl.ds(0, channels * height), :] = source.astype(F32).reshape(channels * height, lon)
        wide[slot, pl.ds(channels * height, (padded - channels) * height), :] = jnp.zeros(
            ((padded - channels) * height, lon), F32
        )

        def row(j):
            return wide[slot, pl.ds(j, padded, stride=height), :].astype(BF16)

        return row

    lanes = lax.broadcasted_iota(jnp.int32, (padded, lon), 1) // (2 * HALO)

    def widen(t, carry):
        pltpu.make_async_copy(
            x_hbm.at[:, pl.ds(t * rows, rows), :], x_ref.at[t], x_sem.at[t]
        ).wait()

        relay(x_ref[t], 0, rows)
        for half in range(rows // HALO):
            beside = jnp.zeros((padded, lon), F32)
            for j in range(HALO):
                r = half * HALO + j
                value = wide[0, pl.ds(r, padded, stride=rows), :]
                xw[t * groups + r // GROUP, :, (r % GROUP) * lon : (r % GROUP + 1) * lon] = value.astype(BF16)
                turn = (2 * j * HALO + HALO) % lon
                beside = jnp.where(lanes == j, pltpu.roll(value, turn, 1), beside)
            cols_send[t * (rows // HALO) + half] = beside.astype(BF16)
        return carry

    lax.fori_loop(0, ahead, widen, 0)
    pl.semaphore_wait(barrier, greetings)
    for copy in direct + spread[: layers - 1]:
        copy.start()
    for copy, dx in zip(row_halo, (1, -1)):
        when_inside(dx, copy.start)

    def send_ready(t, carry):
        send_strips(t)
        return carry

    lax.fori_loop(0, ahead, send_ready, 0)

    def widen_and_send(t, carry):
        @pl.when(t > ahead)
        def _():
            send_strips(t - 1)

        return widen(t, carry)

    lax.fori_loop(ahead, tiles, widen_and_send, 0)
    send_strips(tiles - 1)
    for n, copy in corners:
        when_inside(1 - 2 * n, copy.start)
    for copy in spread[layers - 1 :]:
        copy.start()

    for copy in local:
        copy.wait()
    w1_wide[...] = jnp.zeros_like(w1_wide)
    w1_wide[:channels, :] = w1_in[...].astype(F32) * 0.5
    w1[...] = w1_wide[...].T[:, :padded].astype(BF16)
    cols[...] = vec_ref[...].T
    average = jnp.mean(w2_in[...].astype(F32), axis=0, keepdims=True)
    for k in range(layers):
        block = pl.ds(pl.multiple_of(lax.rem(me + k, layers) * shard, shard), shard)
        w2[pl.ds(k * shard, shard), :] = (w2_in[block, :].astype(F32) - average).astype(BF16)
    e2_wide = e2_in[...].astype(F32)
    e2_ref[...] = (e2_wide - jnp.mean(e2_wide, axis=0, keepdims=True)).astype(BF16)
    tile = lax.axis_index("gx") * lax.axis_size("gy") + lax.axis_index("gy")
    slot_ids = lax.broadcasted_iota(jnp.int32, (1, slots), 1)
    near_ref[...] = jnp.where(slot_ids < count_ref[...], receivers_ref[...] - tile * nodes, -1)
    block, lane = locate(senders_ref[:, own_edges], lat, lon, sides)
    place_ref[0:1, :] = block
    place_ref[2:3, :] = near_ref[:, own_edges]
    cmask[...] = onehot_of(lane, 0, lon)
    b1 = cols[:, 0:1] * 0.5

    def pick_rows(first, count):
        picks = []
        for r in range(count):
            here = jnp.where(place_ref[0:1, :] == first + r, 1.0, 0.0)
            here = jnp.broadcast_to(here, (16, share)).astype(BF16)
            picks.append((cmask[...].reshape(lon // 16, 16, share) * here[None]).reshape(lon, share))
        return jnp.concatenate(picks, axis=0)

    def first_layer(g):
        half = jnp.dot(w1[...], xw[g], preferred_element_type=F32) + b1
        return half_silu(half).astype(BF16)

    own_gain = cols[mine, 1:2]

    def embed(start, stop):
        hidden = first_layer(start * groups)
        for g in range(start * groups, stop * groups):
            t, group = g // groups, g % groups
            pre = jnp.dot(w2[...], hidden, preferred_element_type=F32)
            if g + 1 < stop * groups:
                hidden = first_layer(g + 1)
            own = pre[:shard, :] * inverse_spread(pre) * own_gain
            for r in range(GROUP):
                out_wide[t, pl.ds(group * GROUP + r, shard, stride=rows), :] = own[
                    :, r * lon : (r + 1) * lon
                ]
            if group + 1 == groups:
                stage[t] = out_wide[t].reshape(shard, rows, lon).astype(BF16)

    picked = jnp.zeros((padded, share), F32)
    for t in range(tiles):
        cells = jnp.concatenate([xw[t * groups + g] for g in range(groups)], axis=1)
        picked = picked + jnp.dot(cells, pick_rows(t * rows, rows), preferred_element_type=F32)
    half_ref[0:padded, :] = picked
    pass_nodes()
    last = (((1,), (1,)), ((), ()))
    degree = jnp.zeros((8, nodes), F32)
    for start in range(0, slots, share):
        chunk = onehot_of(near_ref[:, start : start + share], 0, nodes)
        ones = jnp.ones((8, share), BF16)
        degree = degree + lax.dot_general(ones, chunk, last, preferred_element_type=F32)
    degree_ref[...] = jnp.maximum(degree, 1.0)
    embed(0, 1)

    for n, copy in enumerate(row_halo):
        when_inside(1 - 2 * n, copy.wait_send)
        when_inside(2 * n - 1, copy.wait_recv)
    for i in range(2):
        row_of = relay(rows_recv[i], 0, HALO)
        for j in range(HALO):
            rows_all[i, :, j * lon : (j + 1) * lon] = row_of(j)
    cells = jnp.concatenate([rows_all[0], rows_all[1]], axis=1)
    half_ref[0:padded, :] += jnp.dot(cells, pick_rows(lat, 2 * HALO), preferred_element_type=F32)
    embed(1, EARLY)

    for t in range(tiles):
        for i in range(len(steps)):
            strips(t, i).wait()
    for n, copy in corners:
        when_inside(1 - 2 * n, copy.wait_send)
        when_inside(2 * n - 1, copy.wait_recv)
    pieces = [cols_recv[side, b] for side in range(sides) for b in range(lat // HALO)]
    pieces += [corner_recv[n, side] for n in range(2) for side in range(sides)]
    cells = jnp.concatenate(pieces, axis=1)
    picked = half_ref[0:padded, :] + jnp.dot(
        cells, pick_rows(lat + 2 * HALO, cells.shape[1] // lon), preferred_element_type=F32
    )
    half = jnp.dot(w1[...], picked.astype(BF16), preferred_element_type=F32) + b1
    hidden = half_silu(half).astype(BF16)
    pre = jnp.dot(w2[...], hidden, preferred_element_type=F32)
    scale = inverse_spread(pre)
    for k in range(layers):
        block = pl.ds(pl.multiple_of(lax.rem(me + k, layers) * shard, shard), shard)
        rows_k = pre[k * shard : (k + 1) * shard, :] * scale * cols[block, 1:2]
        sender_ref[block, :] = rows_k.astype(BF16)
    half_ref[...] = jnp.dot(e1_ref[:, latent : 2 * latent], sender_ref[...], preferred_element_type=F32)

    receive_nodes()
    onehot = onehot_of(place_ref[2:3, :], 0, nodes)
    mesh_cols = jnp.dot(nodes_all[...], onehot, preferred_element_type=F32).astype(BF16)
    half_ref[...] += jnp.dot(e1_ref[:, 2 * latent :], mesh_cols, preferred_element_type=F32) + cols[:, 2:3]

    for c in range(PARTS):
        for peer in order:
            at = pl.ds(pl.multiple_of(peer * shard, shard), shard)
            to_layer(
                edge_hbm.at[:, pl.ds(0, part)], assigned.at[at, pl.ds(c * part, part)],
                z_send.at[c, 0], z_recv.at[c, peer], peer,
            ).wait_recv()
        at = slice(c * part, (c + 1) * part)
        half = half_ref[:, at] + jnp.dot(e1_ref[:, :latent], assigned[:, at], preferred_element_type=F32)
        hidden = half_silu(half * 0.5).astype(BF16)
        second = jnp.dot(e2_ref[...], hidden, preferred_element_type=F32)
        message = (
            assigned[:, at].astype(F32) + second * inverse_spread(second) * cols[:, 3:4] + cols[:, 4:5]
        ).astype(BF16)
        onehot = onehot_of(place_ref[2:3, at], 0, nodes)
        sums = lax.dot_general(message, onehot, last, preferred_element_type=F32)
        totals[...] = sums if c == 0 else totals[...] + sums
    sent[...] = totals[...].astype(BF16)
    exchange = []
    for k, peer in enumerate(order):
        theirs = pl.ds(pl.multiple_of(peer * shard, shard), shard)
        exchange.append(
            to_layer(sent.at[theirs, :], parts.at[me], z_send.at[PARTS, k], z_recv.at[PARTS, me], peer)
        )
    for copy in exchange:
        copy.start()
    sent_nodes()
    for copy in spread:
        copy.wait_send()

    embed(EARLY, tiles)

    for copy in exchange:
        copy.wait_send()
    total = totals[mine, :]
    for peer in order:
        to_layer(
            sent.at[pl.ds(0, shard), :], parts.at[peer], z_send.at[PARTS, 0], z_recv.at[PARTS, peer], peer
        ).wait_recv()
    for peer in order:
        total = total + parts[peer].astype(F32)
    mean_ref[...] = (nodes_all[mine, :].astype(F32) + total / degree_ref[0:1, :]).astype(BF16)


def finish(stage, mesh_ref, grid_out, mesh_out, sem):
    tiles, _, rows, _ = stage.shape
    copies = [
        pltpu.make_async_copy(stage.at[t], grid_out.at[:, pl.ds(t * rows, rows), :], sem.at[t])
        for t in range(tiles)
    ]
    copies.append(pltpu.make_async_copy(mesh_ref, mesh_out, sem.at[tiles]))
    for copy in copies:
        copy.start()
    for copy in copies:
        copy.wait()


def on_device(
    grid_inputs,
    embed_w1,
    embed_b1,
    embed_w2,
    embed_gain,
    edge_w1,
    edge_b1,
    edge_w2,
    message_gain,
    message_bias,
    mesh_latent,
    edge_latent,
    senders,
    receivers,
    edge_counts,
):
    latent = embed_w2.shape[0]
    channels, lat, lon = grid_inputs.shape
    shard = mesh_latent.shape[0]
    nodes = mesh_latent.shape[3]
    slots = edge_latent.shape[3]
    layers = lax.axis_size("gz")
    sides = 1 if lax.axis_size("gy") == 2 else 2
    share = slots // layers
    padded = -(-channels // 16) * 16
    tiles = lat // ROWS
    I32 = jnp.int32

    vmem = pl.BlockSpec(memory_space=pltpu.VMEM)
    hbm = pl.BlockSpec(memory_space=pltpu.HBM)
    scratch = [
        ((tiles, channels, ROWS, lon), BF16),
        ((1, padded * ROWS, lon), F32),
        ((lat // GROUP, padded, GROUP * lon), BF16),
        ((channels, latent), BF16),
        ((-(-padded // 128) * 128, latent), F32),
        ((latent, padded), BF16),
        (embed_w2.shape, BF16),
        (embed_w2.shape, BF16),
        (edge_w1.shape, BF16),
        (edge_w2.shape, BF16),
        (edge_w2.shape, BF16),
        ((8, latent), F32),
        ((latent, 8), F32),
        ((1, slots), I32),
        ((1, slots), I32),
        ((1, 1), I32),
        ((1, slots), I32),
        ((8, share), I32),
        ((lon, share), BF16),
        ((tiles, shard * ROWS, lon), F32),
        ((latent, share), BF16),
        ((latent, share), F32),
        ((lat // HALO, padded, lon), BF16),
        ((2, channels, HALO, lon), BF16),
        ((2, padded, HALO * lon), BF16),
        ((sides, lat // HALO, padded, lon), BF16),
        ((2, sides, padded, lon), BF16),
        ((latent, share), BF16),
        ((latent, nodes), BF16),
        ((latent, nodes), F32),
        ((latent, nodes), BF16),
        ((layers, shard, nodes), BF16),
        ((8, nodes), F32),
    ]
    sems = [(tiles,), (14,), (8,), (8,), (sides, tiles), (sides, tiles), (PARTS + 1, layers), (PARTS + 1, layers), (layers + 1,), (layers,)]
    line = lambda v: v.reshape(1, v.size)
    stage, mean = pl.pallas_call(
        kernel,
        in_specs=[hbm] * 15,
        out_specs=[vmem, vmem],
        out_shape=[
            pltpu.VMEM((tiles, shard, ROWS, lon), BF16),
            pltpu.VMEM((shard, nodes), BF16),
        ],
        scratch_shapes=[pltpu.VMEM(s, d) for s, d in scratch]
        + [pltpu.SemaphoreType.DMA(s) for s in sems],
        compiler_params=pltpu.CompilerParams(
            collective_id=0, has_side_effects=True, vmem_limit_bytes=64_860_000
        ),
    )(
        grid_inputs, embed_w1.T, embed_w2, edge_w1, edge_w2,
        line(embed_b1), line(embed_gain), line(edge_b1), line(message_gain), line(message_bias),
        mesh_latent[:, 0, 0, :], edge_latent[:, 0, 0, :], line(senders), line(receivers), edge_counts,
    )
    grid_out, mesh_out = pl.pallas_call(
        finish,
        in_specs=[vmem, vmem],
        out_specs=[hbm, hbm],
        out_shape=[
            jax.ShapeDtypeStruct((shard, lat, lon), BF16),
            jax.ShapeDtypeStruct((shard, nodes), BF16),
        ],
        scratch_shapes=[pltpu.SemaphoreType.DMA((tiles + 1,))],
        compiler_params=pltpu.CompilerParams(vmem_limit_bytes=1024 * 1024),
    )(
        pltpu.with_memory_space_constraint(stage, pltpu.VMEM),
        pltpu.with_memory_space_constraint(mean, pltpu.VMEM),
    )
    return (mesh_out.reshape(shard, 1, 1, nodes), grid_out)


def solution(mesh):
    return jax.shard_map(
        on_device,
        mesh=mesh,
        in_specs=(
            P(None, "gx", "gy"),
            P(),
            P(),
            P(),
            P(),
            P(),
            P(),
            P(),
            P(),
            P(),
            P("gz", "gx", "gy", None),
            P("gz", "gx", "gy", None),
            P("gx", "gy", None),
            P("gx", "gy", None),
            P("gx", "gy"),
        ),
        out_specs=(P("gz", "gx", "gy", None), P("gz", "gx", "gy")),
        check_vma=False,
    )
```

```python
import jax
import jax.numpy as jnp
from jax import lax
from jax.experimental import pallas as pl
from jax.experimental.pallas import tpu as pltpu
from jax.sharding import PartitionSpec as P

HALO = 8
ROWS = 16
GROUP = 4
EARLY = 2
PARTS = 2

epsilon = 1e-05
F32 = jnp.float32
BF16 = jnp.bfloat16
MESH = pl.DeviceIdType.MESH


def half_silu(half):
    return half + half * jnp.tanh(half)


def inverse_spread(values):
    return lax.rsqrt(jnp.mean(values * values, axis=0, keepdims=True) + epsilon)


def onehot_of(index_row, first, count):
    ids = lax.broadcasted_iota(jnp.int32, (count, index_row.shape[1]), 0)
    return jnp.where(ids == index_row - first, 1.0, 0.0).astype(BF16)


def partner(dx, dy, dz):
    ids = {}
    for axis, step in (("gx", dx), ("gy", dy), ("gz", dz)):
        size = lax.axis_size(axis)
        ids[axis] = lax.rem(lax.axis_index(axis) + (step + size), size)
    return ids


def remote(source, target, send_sem, recv_sem, offset):
    return pltpu.make_async_remote_copy(
        src_ref=source, dst_ref=target, send_sem=send_sem, recv_sem=recv_sem,
        device_id=partner(*offset), device_id_type=MESH,
    )


def split(values, size):
    if size & (size - 1) == 0:
        return lax.shift_right_logical(values, size.bit_length() - 1), values & (size - 1)
    return values // size, values % size


def locate(send, lat, lon, sides):
    band = lax.axis_index("gx")
    sector = lax.axis_index("gy")
    lon_total = lon * lax.axis_size("gy")
    row, column = split(send, lon_total)
    row = row - band * lat
    column = split(column - sector * lon + (HALO + lon_total), lon_total)[1] - HALO
    above, below = row < 0, row >= lat
    west, east = column < 0, column >= lon
    outside_row = jnp.where(above, 1, jnp.where(below, 1, 0))
    outside_column = jnp.where(west, 1, jnp.where(east, 1, 0))
    tall = lat // HALO
    side = jnp.where(west, 0, sides - 1)
    beside = jnp.where(west, column + HALO, column - lon + HALO)
    row_block = lat + jnp.where(above, row + HALO, row - lat + HALO)
    column_block = lat + 2 * HALO + side * tall + lax.shift_right_arithmetic(row, HALO.bit_length() - 1)
    corner_block = lat + 2 * HALO + sides * tall + jnp.where(above, 0, 1) * sides + side
    block = jnp.where(
        outside_column == 0,
        jnp.where(outside_row == 0, row, row_block),
        jnp.where(outside_row == 0, column_block, corner_block),
    )
    lane = jnp.where(outside_column == 0, column, (row & (HALO - 1)) * (2 * HALO) + beside)
    return block, lane


def kernel(
    x_hbm, w1_hbm, w2_hbm, e1_hbm, e2_hbm, b1_hbm, gain_hbm, eb1_hbm, mgain_hbm, mbias_hbm,
    mesh_hbm, edge_hbm, senders_hbm, receivers_hbm, count_hbm,
    stage, mean_ref,
    x_ref, wide, xw, w1_in, w1_wide, w1, w2_in, w2, e1_ref, e2_in, e2_ref, vec_ref, cols,
    senders_ref, receivers_ref, count_ref, near_ref, place_ref, cmask, out_wide, sender_ref, half_ref,
    cols_send, rows_recv, rows_all, cols_recv, corner_recv,
    assigned, nodes_all, totals, sent, parts, degree_ref,
    x_sem, in_sem, halo_send, halo_recv, col_send, col_recv, z_send, z_recv, n_send, n_recv,
):
    tiles, channels, rows, lon = x_ref.shape
    lat = tiles * rows
    padded = w1.shape[1]
    latent, share = assigned.shape
    shard, nodes = parts.shape[1:]
    slots = receivers_ref.shape[1]
    layers = slots // share
    sides = cols_recv.shape[0]
    groups = rows // GROUP
    me = lax.axis_index("gz")
    mine = pl.ds(pl.multiple_of(me * shard, shard), shard)
    own_edges = pl.ds(pl.multiple_of(me * share, share), share)

    steps = (1,) if sides == 1 else (-1, 1)
    bands = lax.axis_size("gx")
    band = lax.axis_index("gx")

    def inside(dx):
        return jnp.logical_and(band + dx >= 0, band + dx < bands)

    def when_inside(dx, action):
        @pl.when(inside(dx))
        def _():
            action()

    barrier = pltpu.get_barrier_semaphore()

    def greet(offset):
        pl.semaphore_signal(barrier, inc=1, device_id=partner(*offset), device_id_type=MESH)

    peers = [(0, 0, k) for k in range(1, layers)] + [(0, dy, 0) for dy in steps]
    for offset in peers:
        greet(offset)
    across = [(0,)] + [(dy,) for dy in steps]
    for dx in (1, -1):
        when_inside(dx, lambda: [greet((dx, *dy, 0)) for dy in across])
    greetings = len(peers) + len(across) * (2 - (band == 0).astype(jnp.int32) - (band == bands - 1).astype(jnp.int32))
    local = [
        (w1_hbm, w1_in), (w2_hbm, w2_in), (senders_hbm, senders_ref), (receivers_hbm, receivers_ref),
        (count_hbm, count_ref), (e1_hbm, e1_ref), (e2_hbm, e2_in),
        (mesh_hbm, nodes_all.at[mine, :]), (edge_hbm.at[:, own_edges], assigned.at[mine, :]),
    ]
    local += [
        (ref, vec_ref.at[pl.ds(i, 1), :])
        for i, ref in enumerate((b1_hbm, gain_hbm, eb1_hbm, mgain_hbm, mbias_hbm))
    ]
    local = [pltpu.make_async_copy(a, b, in_sem.at[i]) for i, (a, b) in enumerate(local)]
    loads = [
        pltpu.make_async_copy(x_hbm.at[:, pl.ds(t * rows, rows), :], x_ref.at[t], x_sem.at[t])
        for t in range(tiles)
    ]
    for load in loads + local:
        load.start()

    half_layers = layers // 2
    side = me // half_layers
    paired = layers == 4
    mate = me + 1 - 2 * lax.rem(me, 2)
    far_peers = [lax.rem((1 - side) * half_layers + j, layers) for j in range(half_layers)]
    near_peers = [side * half_layers + lax.rem(me + j, half_layers) for j in range(1, half_layers)]
    order = far_peers + near_peers
    if 2 * half_layers != layers:
        order = [lax.rem(me + k, layers) for k in range(1, layers)]

    def to_layer(source, target, send_sem, recv_sem, peer):
        return pltpu.make_async_remote_copy(
            src_ref=source, dst_ref=target, send_sem=send_sem, recv_sem=recv_sem,
            device_id={"gz": peer}, device_id_type=MESH,
        )

    def nodes_to(block, peer, slot, source):
        at = pl.ds(pl.multiple_of(block * shard, shard), shard)
        return to_layer(source, nodes_all.at[at, :], n_send.at[slot], n_recv.at[block], peer)

    if paired:
        direct = [nodes_to(me, peer, i, mesh_hbm) for i, peer in enumerate((2 - side, mate))]
    else:
        direct = [nodes_to(me, peer, i, mesh_hbm) for i, peer in enumerate(order)]
    is_hub = jnp.logical_and(me > 0, me < layers - 1)

    def passed():
        return [
            nodes_to(block, mate, 2 + i, nodes_all.at[pl.ds(pl.multiple_of(block * shard, shard), shard), :])
            for i, block in enumerate(far_peers)
        ]

    def pass_nodes():
        if paired:
            @pl.when(is_hub)
            def _():
                for copy in passed():
                    copy.wait_recv()
                    copy.start()

    def receive_nodes():
        for i, block in enumerate(near_peers if paired else order):
            nodes_to(block, mate, i, mesh_hbm).wait_recv()
        if paired:
            @pl.when(jnp.logical_not(is_hub))
            def _():
                for copy in passed():
                    copy.wait_recv()

    def sent_nodes():
        for copy in direct:
            copy.wait_send()
        if paired:
            @pl.when(is_hub)
            def _():
                for copy in passed():
                    copy.wait_send()

    part = share // PARTS
    spread = []
    for c in range(PARTS):
        for k, peer in enumerate(order):
            theirs = pl.ds(pl.multiple_of(peer * share + c * part, part), part)
            spread.append(
                to_layer(
                    edge_hbm.at[:, theirs], assigned.at[mine, pl.ds(c * part, part)],
                    z_send.at[c, k], z_recv.at[c, me], peer,
                )
            )
    row_halo = [
        remote(x_hbm.at[:, pl.ds(lat - HALO, HALO), :], rows_recv.at[0], halo_send.at[0], halo_recv.at[0], (1, 0, 0)),
        remote(x_hbm.at[:, pl.ds(0, HALO), :], rows_recv.at[1], halo_send.at[1], halo_recv.at[1], (-1, 0, 0)),
    ]
    corners = []
    for i, dy in enumerate(steps):
        slot = sides - 1 - i
        for n, dx in enumerate((1, -1)):
            block = cols_send.at[lat // HALO - 1 if dx > 0 else 0]
            at = 2 + 2 * n + i
            corners.append(
                (n, remote(block, corner_recv.at[n, slot], halo_send.at[at], halo_recv.at[at], (dx, dy, 0)))
            )

    def fill(n):
        rows_recv[n] = jnp.zeros(rows_recv.shape[1:], BF16)
        corner_recv[n] = jnp.zeros(corner_recv.shape[1:], BF16)

    pl.when(band == 0)(lambda: fill(0))
    pl.when(band == bands - 1)(lambda: fill(1))

    def strips(t, i):
        blocks = pl.ds(t * (rows // HALO), rows // HALO)
        return remote(
            cols_send.at[blocks], cols_recv.at[sides - 1 - i, blocks],
            col_send.at[i, t], col_recv.at[i, t], (0, steps[i], 0),
        )

    def send_strips(t):
        for i in range(len(steps)):
            strips(t, i).start()

    ahead = jnp.maximum(tiles - 1 - me - jnp.minimum(lax.axis_index("gy"), 1), 0)

    def relay(source, slot, height):
        wide[slot, pl.ds(0, channels * height), :] = source.astype(F32).reshape(channels * height, lon)
        wide[slot, pl.ds(channels * height, (padded - channels) * height), :] = jnp.zeros(
            ((padded - channels) * height, lon), F32
        )

        def row(j):
            return wide[slot, pl.ds(j, padded, stride=height), :].astype(BF16)

        return row

    lanes = lax.broadcasted_iota(jnp.int32, (padded, lon), 1) // (2 * HALO)

    def widen(t, carry):
        pltpu.make_async_copy(
            x_hbm.at[:, pl.ds(t * rows, rows), :], x_ref.at[t], x_sem.at[t]
        ).wait()

        relay(x_ref[t], 0, rows)
        for half in range(rows // HALO):
            beside = jnp.zeros((padded, lon), F32)
            for j in range(HALO):
                r = half * HALO + j
                value = wide[0, pl.ds(r, padded, stride=rows), :]
                xw[t * groups + r // GROUP, :, (r % GROUP) * lon : (r % GROUP + 1) * lon] = value.astype(BF16)
                turn = (2 * j * HALO + HALO) % lon
                beside = jnp.where(lanes == j, pltpu.roll(value, turn, 1), beside)
            cols_send[t * (rows // HALO) + half] = beside.astype(BF16)
        return carry

    lax.fori_loop(0, ahead, widen, 0)
    pl.semaphore_wait(barrier, greetings)
    for copy in direct + spread[: layers - 1]:
        copy.start()
    for copy, dx in zip(row_halo, (1, -1)):
        when_inside(dx, copy.start)

    def send_ready(t, carry):
        send_strips(t)
        return carry

    lax.fori_loop(0, ahead, send_ready, 0)

    def widen_and_send(t, carry):
        @pl.when(t > ahead)
        def _():
            send_strips(t - 1)

        return widen(t, carry)

    lax.fori_loop(ahead, tiles, widen_and_send, 0)
    send_strips(tiles - 1)
    for n, copy in corners:
        when_inside(1 - 2 * n, copy.start)
    for copy in spread[layers - 1 :]:
        copy.start()

    for copy in local:
        copy.wait()
    w1_wide[...] = jnp.zeros_like(w1_wide)
    w1_wide[:channels, :] = w1_in[...].astype(F32) * 0.5
    w1[...] = w1_wide[...].T[:, :padded].astype(BF16)
    cols[...] = vec_ref[...].T
    average = jnp.mean(w2_in[...].astype(F32), axis=0, keepdims=True)
    for k in range(layers):
        block = pl.ds(pl.multiple_of(lax.rem(me + k, layers) * shard, shard), shard)
        w2[pl.ds(k * shard, shard), :] = (w2_in[block, :].astype(F32) - average).astype(BF16)
    e2_wide = e2_in[...].astype(F32)
    e2_ref[...] = (e2_wide - jnp.mean(e2_wide, axis=0, keepdims=True)).astype(BF16)
    tile = lax.axis_index("gx") * lax.axis_size("gy") + lax.axis_index("gy")
    slot_ids = lax.broadcasted_iota(jnp.int32, (1, slots), 1)
    near_ref[...] = jnp.where(slot_ids < count_ref[...], receivers_ref[...] - tile * nodes, -1)
    block, lane = locate(senders_ref[:, own_edges], lat, lon, sides)
    place_ref[0:1, :] = block
    place_ref[2:3, :] = near_ref[:, own_edges]
    cmask[...] = onehot_of(lane, 0, lon)
    b1 = cols[:, 0:1] * 0.5

    def pick_rows(first, count):
        picks = []
        for r in range(count):
            here = jnp.where(place_ref[0:1, :] == first + r, 1.0, 0.0)
            here = jnp.broadcast_to(here, (16, share)).astype(BF16)
            picks.append((cmask[...].reshape(lon // 16, 16, share) * here[None]).reshape(lon, share))
        return jnp.concatenate(picks, axis=0)

    def first_layer(g):
        half = jnp.dot(w1[...], xw[g], preferred_element_type=F32) + b1
        return half_silu(half).astype(BF16)

    own_gain = cols[mine, 1:2]

    def embed(start, stop):
        hidden = first_layer(start * groups)
        for g in range(start * groups, stop * groups):
            t, group = g // groups, g % groups
            pre = jnp.dot(w2[...], hidden, preferred_element_type=F32)
            if g + 1 < stop * groups:
                hidden = first_layer(g + 1)
            own = pre[:shard, :] * inverse_spread(pre) * own_gain
            for r in range(GROUP):
                out_wide[t, pl.ds(group * GROUP + r, shard, stride=rows), :] = own[
                    :, r * lon : (r + 1) * lon
                ]
            if group + 1 == groups:
                stage[t] = out_wide[t].reshape(shard, rows, lon).astype(BF16)

    picked = jnp.zeros((padded, share), F32)
    for t in range(tiles):
        cells = jnp.concatenate([xw[t * groups + g] for g in range(groups)], axis=1)
        picked = picked + jnp.dot(cells, pick_rows(t * rows, rows), preferred_element_type=F32)
    half_ref[0:padded, :] = picked
    pass_nodes()
    last = (((1,), (1,)), ((), ()))
    degree = jnp.zeros((8, nodes), F32)
    for start in range(0, slots, share):
        chunk = onehot_of(near_ref[:, start : start + share], 0, nodes)
        ones = jnp.ones((8, share), BF16)
        degree = degree + lax.dot_general(ones, chunk, last, preferred_element_type=F32)
    degree_ref[...] = jnp.maximum(degree, 1.0)
    embed(0, 1)

    for n, copy in enumerate(row_halo):
        when_inside(1 - 2 * n, copy.wait_send)
        when_inside(2 * n - 1, copy.wait_recv)
    for i in range(2):
        row_of = relay(rows_recv[i], 0, HALO)
        for j in range(HALO):
            rows_all[i, :, j * lon : (j + 1) * lon] = row_of(j)
    cells = jnp.concatenate([rows_all[0], rows_all[1]], axis=1)
    half_ref[0:padded, :] += jnp.dot(cells, pick_rows(lat, 2 * HALO), preferred_element_type=F32)
    embed(1, EARLY)

    for t in range(tiles):
        for i in range(len(steps)):
            strips(t, i).wait()
    for n, copy in corners:
        when_inside(1 - 2 * n, copy.wait_send)
        when_inside(2 * n - 1, copy.wait_recv)
    pieces = [cols_recv[side, b] for side in range(sides) for b in range(lat // HALO)]
    pieces += [corner_recv[n, side] for n in range(2) for side in range(sides)]
    cells = jnp.concatenate(pieces, axis=1)
    picked = half_ref[0:padded, :] + jnp.dot(
        cells, pick_rows(lat + 2 * HALO, cells.shape[1] // lon), preferred_element_type=F32
    )
    half = jnp.dot(w1[...], picked.astype(BF16), preferred_element_type=F32) + b1
    hidden = half_silu(half).astype(BF16)
    pre = jnp.dot(w2[...], hidden, preferred_element_type=F32)
    scale = inverse_spread(pre)
    for k in range(layers):
        block = pl.ds(pl.multiple_of(lax.rem(me + k, layers) * shard, shard), shard)
        rows_k = pre[k * shard : (k + 1) * shard, :] * scale * cols[block, 1:2]
        sender_ref[block, :] = rows_k.astype(BF16)
    half_ref[...] = jnp.dot(e1_ref[:, latent : 2 * latent], sender_ref[...], preferred_element_type=F32)

    receive_nodes()
    onehot = onehot_of(place_ref[2:3, :], 0, nodes)
    mesh_cols = jnp.dot(nodes_all[...], onehot, preferred_element_type=F32).astype(BF16)
    half_ref[...] += jnp.dot(e1_ref[:, 2 * latent :], mesh_cols, preferred_element_type=F32) + cols[:, 2:3]

    for c in range(PARTS):
        for peer in order:
            at = pl.ds(pl.multiple_of(peer * shard, shard), shard)
            to_layer(
                edge_hbm.at[:, pl.ds(0, part)], assigned.at[at, pl.ds(c * part, part)],
                z_send.at[c, 0], z_recv.at[c, peer], peer,
            ).wait_recv()
        at = slice(c * part, (c + 1) * part)
        half = half_ref[:, at] + jnp.dot(e1_ref[:, :latent], assigned[:, at], preferred_element_type=F32)
        hidden = half_silu(half * 0.5).astype(BF16)
        second = jnp.dot(e2_ref[...], hidden, preferred_element_type=F32)
        message = (
            assigned[:, at].astype(F32) + second * inverse_spread(second) * cols[:, 3:4] + cols[:, 4:5]
        ).astype(BF16)
        onehot = onehot_of(place_ref[2:3, at], 0, nodes)
        sums = lax.dot_general(message, onehot, last, preferred_element_type=F32)
        totals[...] = sums if c == 0 else totals[...] + sums
    sent[...] = totals[...].astype(BF16)
    exchange = []
    for k, peer in enumerate(order):
        theirs = pl.ds(pl.multiple_of(peer * shard, shard), shard)
        exchange.append(
            to_layer(sent.at[theirs, :], parts.at[me], z_send.at[PARTS, k], z_recv.at[PARTS, me], peer)
        )
    for copy in exchange:
        copy.start()
    sent_nodes()
    for copy in spread:
        copy.wait_send()

    embed(EARLY, tiles)

    for copy in exchange:
        copy.wait_send()
    total = totals[mine, :]
    for peer in order:
        to_layer(
            sent.at[pl.ds(0, shard), :], parts.at[peer], z_send.at[PARTS, 0], z_recv.at[PARTS, peer], peer
        ).wait_recv()
    for peer in order:
        total = total + parts[peer].astype(F32)
    mean_ref[...] = (nodes_all[mine, :].astype(F32) + total / degree_ref[0:1, :]).astype(BF16)


def finish(stage, mesh_ref, grid_out, mesh_out, sem):
    tiles, _, rows, _ = stage.shape
    copies = [
        pltpu.make_async_copy(stage.at[t], grid_out.at[:, pl.ds(t * rows, rows), :], sem.at[t])
        for t in range(tiles)
    ]
    copies.append(pltpu.make_async_copy(mesh_ref, mesh_out, sem.at[tiles]))
    for copy in copies:
        copy.start()
    for copy in copies:
        copy.wait()


def on_device(
    grid_inputs,
    embed_w1,
    embed_b1,
    embed_w2,
    embed_gain,
    edge_w1,
    edge_b1,
    edge_w2,
    message_gain,
    message_bias,
    mesh_latent,
    edge_latent,
    senders,
    receivers,
    edge_counts,
):
    latent = embed_w2.shape[0]
    channels, lat, lon = grid_inputs.shape
    shard = mesh_latent.shape[0]
    nodes = mesh_latent.shape[3]
    slots = edge_latent.shape[3]
    layers = lax.axis_size("gz")
    sides = 1 if lax.axis_size("gy") == 2 else 2
    share = slots // layers
    padded = -(-channels // 16) * 16
    tiles = lat // ROWS
    I32 = jnp.int32

    vmem = pl.BlockSpec(memory_space=pltpu.VMEM)
    hbm = pl.BlockSpec(memory_space=pltpu.HBM)
    scratch = [
        ((tiles, channels, ROWS, lon), BF16),
        ((1, padded * ROWS, lon), F32),
        ((lat // GROUP, padded, GROUP * lon), BF16),
        ((channels, latent), BF16),
        ((-(-padded // 128) * 128, latent), F32),
        ((latent, padded), BF16),
        (embed_w2.shape, BF16),
        (embed_w2.shape, BF16),
        (edge_w1.shape, BF16),
        (edge_w2.shape, BF16),
        (edge_w2.shape, BF16),
        ((8, latent), F32),
        ((latent, 8), F32),
        ((1, slots), I32),
        ((1, slots), I32),
        ((1, 1), I32),
        ((1, slots), I32),
        ((8, share), I32),
        ((lon, share), BF16),
        ((tiles, shard * ROWS, lon), F32),
        ((latent, share), BF16),
        ((latent, share), F32),
        ((lat // HALO, padded, lon), BF16),
        ((2, channels, HALO, lon), BF16),
        ((2, padded, HALO * lon), BF16),
        ((sides, lat // HALO, padded, lon), BF16),
        ((2, sides, padded, lon), BF16),
        ((latent, share), BF16),
        ((latent, nodes), BF16),
        ((latent, nodes), F32),
        ((latent, nodes), BF16),
        ((layers, shard, nodes), BF16),
        ((8, nodes), F32),
    ]
    sems = [(tiles,), (14,), (8,), (8,), (sides, tiles), (sides, tiles), (PARTS + 1, layers), (PARTS + 1, layers), (layers + 1,), (layers,)]
    line = lambda v: v.reshape(1, v.size)
    stage, mean = pl.pallas_call(
        kernel,
        in_specs=[hbm] * 15,
        out_specs=[vmem, vmem],
        out_shape=[
            pltpu.VMEM((tiles, shard, ROWS, lon), BF16),
            pltpu.VMEM((shard, nodes), BF16),
        ],
        scratch_shapes=[pltpu.VMEM(s, d) for s, d in scratch]
        + [pltpu.SemaphoreType.DMA(s) for s in sems],
        compiler_params=pltpu.CompilerParams(
            collective_id=0, has_side_effects=True, vmem_limit_bytes=64_860_000
        ),
    )(
        grid_inputs, embed_w1.T, embed_w2, edge_w1, edge_w2,
        line(embed_b1), line(embed_gain), line(edge_b1), line(message_gain), line(message_bias),
        mesh_latent[:, 0, 0, :], edge_latent[:, 0, 0, :], line(senders), line(receivers), edge_counts,
    )
    grid_out, mesh_out = pl.pallas_call(
        finish,
        in_specs=[vmem, vmem],
        out_specs=[hbm, hbm],
        out_shape=[
            jax.ShapeDtypeStruct((shard, lat, lon), BF16),
            jax.ShapeDtypeStruct((shard, nodes), BF16),
        ],
        scratch_shapes=[pltpu.SemaphoreType.DMA((tiles + 1,))],
        compiler_params=pltpu.CompilerParams(vmem_limit_bytes=1024 * 1024),
    )(
        pltpu.with_memory_space_constraint(stage, pltpu.VMEM),
        pltpu.with_memory_space_constraint(mean, pltpu.VMEM),
    )
    return (mesh_out.reshape(shard, 1, 1, nodes), grid_out)


def solution(mesh):
    return jax.shard_map(
        on_device,
        mesh=mesh,
        in_specs=(
            P(None, "gx", "gy"),
            P(),
            P(),
            P(),
            P(),
            P(),
            P(),
            P(),
            P(),
            P(),
            P("gz", "gx", "gy", None),
            P("gz", "gx", "gy", None),
            P("gx", "gy", None),
            P("gx", "gy", None),
            P("gx", "gy"),
        ),
        out_specs=(P("gz", "gx", "gy", None), P("gz", "gx", "gy")),
        check_vma=False,
    )
```
